256 devices in a mesh: dom: 16 (over z_lo, y, core), rep: 16 (over x, z_hi).
Axes of the slice: x: 4, y: 4, z: 8 (z_hi: 4, z_lo: 2; z = z_hi * 2 + z_lo), core: 2. Of those that a mesh axis runs over, the one named last changes fastest.
Arguments:
- facts: float32 [1048576, 256], P(('dom', 'rep')), may hold values from -6 to 6
- row_owner: int32 [1048576, 1], P(('dom', 'rep')), may hold values from 0 to 15; in each aligned block of 4096 rows (0 to 4095, 4096 to 8191, ...) at most 512 rows name the same one
- key_offset: int32 [1048576], P(('dom', 'rep')), may hold values from 0 to 255
Outputs:
- key_means: float32 [4096, 256], P(('dom', 'rep'))
- key_counts: float32 [4096], P(('dom', 'rep'))
The draws below stay inside these ranges and needn't reach their ends.
Inputs may be any that keep to these rules, and one draw needn't show every extreme that they name: `row_owner`: in the rows of one device no key range is named by more than 512 rows, a bound that some block reaches.
All inputs are finite; a program needn't handle non-finite values.
Results may differ from the reference program's by a relative error of at most 0.0003.
Values sent between devices are 32-bit elements; how exact they have to be, the bound alone decides.
A program may use at most 64 MiB of HBM per device.

```python
import math
import jax
import jax.numpy as jnp
import numpy as np

M = 256
KEYS = 4096
ROWS_DEV = 4096
ROWS = 1048576
RANGE = 256
CAP = 512
N_DOM = 16


def draw_key_offset(key, part):
    order_key = jax.random.fold_in(key, 11)
    kept_key = jax.random.fold_in(key, 12)
    first_key = jax.random.fold_in(key, 13)
    second_key = jax.random.fold_in(key, 14)
    inner_offsets = (jax.random.permutation(order_key, RANGE - 2) + 1).astype(jnp.int32)
    end_offsets = jnp.array([0, RANGE - 1], jnp.int32)
    kept_offsets = jnp.concatenate([end_offsets, inner_offsets[4:]])
    kept_offsets = jax.random.permutation(kept_key, kept_offsets).astype(jnp.int32)
    first_draw = jax.random.randint(first_key, (ROWS,), 0, RANGE - 4, dtype=jnp.int32)
    second_draw = jax.random.randint(second_key, (ROWS,), 0, RANGE - 4, dtype=jnp.int32)
    return kept_offsets[jnp.minimum(first_draw, second_draw)].astype(jnp.int32)


def block_levels(rng, shape, shards, least, top_value):
    factor_of = 1.0
    for axis_at, parts in shards:
        steps = jax.random.uniform(jax.random.fold_in(jax.random.fold_in(rng, 6), axis_at), (parts,), jnp.float32, least / len(shards), top_value / len(shards))
        factor_of = factor_of * jnp.repeat(jnp.exp(steps), shape[axis_at] // parts).reshape((-1,) + (1,) * (len(shape) - 1 - axis_at))
    return factor_of


def shared_out(stream_key, own, number, rows, amount, top, reach, skew):
    order = jax.random.permutation(stream_key, amount)
    packed, usual = shares(amount, rows * top, reach, skew, True), shares(amount, rows * top, reach, skew, False)
    places = jnp.arange(amount)

    def named(tallies, rotation):
        used = int((tallies > 0).sum())
        fixed = max(1, used // 4)
        shifted = fixed + (places - fixed + rotation * (used - fixed)) % max(1, amount - fixed)
        return jnp.zeros((amount,), jnp.int32).at[order[jnp.where(places < fixed, places, shifted)]].set(jnp.asarray(tallies, jnp.int32))

    tallies = jnp.where(number % 4 == 0, named(packed, number // 4), named(usual, number - number // 4 - 1))
    mixed = jax.random.permutation(jax.random.fold_in(own, 3), amount)
    source_of, taker = mixed[0:amount // 2 * 2:2], mixed[1:amount // 2 * 2:2]
    slack = jnp.minimum(tallies[source_of] - 1, reach - tallies[taker]) // 2
    slack = jnp.where((source_of == order[0]) | (taker == order[0]) | (tallies[taker] == 0), 0, jnp.maximum(slack, 0))
    shifted = jax.random.randint(jax.random.fold_in(own, 4), (amount // 2,), 0, 1 << 20) % (slack + 1)
    tallies = tallies.at[source_of].add(-shifted).at[taker].add(shifted)
    items = jnp.searchsorted(jnp.cumsum(tallies), jnp.arange(rows * top), side="right").astype(jnp.int32)
    grid = items.reshape(top, rows).T
    grid = grid[jax.random.permutation(jax.random.fold_in(own, 1), rows)]
    rotation = jax.random.randint(jax.random.fold_in(own, 2), (rows, 1), 0, top)
    return jnp.take_along_axis(grid, (jnp.arange(top)[None, :] + rotation) % top, axis=1)


def shares(count, total, most, slope, full):
    portions = [(1 << 20) // math.isqrt(grade ** slope) + 1 for grade in range(1, count + 1)]
    largest = most if full else min(most, max(-(-total // count), total * portions[0] // sum(portions)))
    least = 1 if total - largest >= count - 1 else 0
    holding, rest = [largest] + [least] * (count - 1), total - largest - least * (count - 1)
    while rest > 0:
        free = [i for i in range(1, count) if holding[i] < largest] or [i for i in range(1, count) if holding[i] < most]
        mass, remaining = sum([portions[i] for i in free]), rest
        for i in free:
            more = min(most - holding[i], max(1, remaining * portions[i] // mass), rest)
            holding[i] = holding[i] + more
            rest = rest - more
    return np.array(holding)


def centred(own_key, extent, deviation, bound, split=(), held_as=jnp.bfloat16):
    result = deviation * jax.random.normal(own_key, extent, jnp.float32)
    if split:
        result = result * block_levels(own_key, extent, split, -0.22, 0.18)
    return jnp.clip(result, -bound, bound).astype(held_as)


def setup_inputs(seed: int = 0) -> dict:
    splits = jax.random.split(jax.random.key(seed), 4)
    facts = centred(splits[0], (ROWS, M), 1.0, 6.0, ((0, 256),), jnp.float32)
    row_owner_keys = jax.random.split(jax.random.fold_in(splits[1], 1), ROWS // ROWS_DEV)
    row_owner_turns = jax.random.permutation(jax.random.fold_in(splits[1], 3), ROWS // ROWS_DEV)
    row_owner = jax.vmap(lambda own, number: shared_out(jax.random.fold_in(splits[1], 2), own, number, ROWS_DEV, N_DOM, 1, CAP, 2))(row_owner_keys, row_owner_turns).reshape((ROWS, 1))
    key_offset = draw_key_offset(jax.random.fold_in(splits[3], 71), 0)
    return dict(facts=facts, row_owner=row_owner, key_offset=key_offset)


def reference(facts, row_owner, key_offset):
    key_ids = row_owner[:, 0] * (KEYS // N_DOM) + key_offset
    key_sums = jax.ops.segment_sum(facts, key_ids, num_segments=KEYS)
    key_counts = jax.ops.segment_sum(jnp.ones(key_ids.shape, jnp.float32), key_ids, num_segments=KEYS)
    key_means = key_sums / jnp.maximum(key_counts, 1.0)[:, None]
    return key_means, key_counts
```

```python
import functools

import jax
import jax.numpy as jnp
from jax import lax
from jax.experimental import pallas as pl
from jax.experimental.pallas import tpu as pltpu
from jax.sharding import PartitionSpec as P

MESH = pl.DeviceIdType.MESH
ROWS = 4096
KEYS = 4096
M = 256
UNITS = 8
F32 = jnp.float32
BF16 = jnp.bfloat16


def when(cond, fn):
    if isinstance(cond, (bool, int)):
        if cond:
            fn()
    else:
        pl.when(cond)(fn)


def rows(start, size):
    return pl.ds(pl.multiple_of(start, size), size)


def kernel(
    ids_ref, facts_ref, means_ref, counts_ref,
    fbuf, hl, own, part, land, xa, xb, ya, yb, yr, yxa, yxb, xr, xya, xyb, fin, zl_buf,
    cnt, cland, czland,
    f_sem, d_s, d_r, xa_s, xa_r, xb_s, xb_r, ya_s, ya_r, yb_s, yb_r,
    yxa_s, yxa_r, yxb_s, yxb_r, xya_s, xya_r, xyb_s, xyb_r, z_s, z_r, c_s, c_r, cz_s, cz_r,
):
    dom, rep = lax.axis_index("dom"), lax.axis_index("rep")
    z_lo, y, core = dom // 8, (dom // 2) % 4, dom % 2
    x, z_hi = rep // 4, rep % 4

    def at(zl=z_lo, yy=y, cc=core, xx=x, zh=z_hi):
        return {"dom": zl * 8 + yy * 2 + cc, "rep": xx * 4 + zh}

    partner = at(cc=1 - core)
    xp, xm = at(xx=(x + 1) % 4), at(xx=(x + 3) % 4)
    yp, ym = at(yy=(y + 1) % 4), at(yy=(y + 3) % 4)

    def z_peer(k):
        z = (z_hi * 2 + z_lo + k) % 8
        return z // 2, z % 2

    peers = [partner, xp, xm, yp, ym]
    for k in range(1, 8):
        zh, zl = z_peer(k)
        peers.append(at(zl=zl, zh=zh))

    barrier = pltpu.get_barrier_semaphore()
    for p in peers:
        pl.semaphore_signal(barrier, inc=1, device_id=p, device_id_type=MESH)

    def rc(src, dst, ss, rs, dev):
        return pltpu.make_async_remote_copy(
            src_ref=src, dst_ref=dst, send_sem=ss, recv_sem=rs, device_id=dev, device_id_type=MESH
        )

    def arrived(buf, ss, rs):
        rc(buf, buf, ss, rs, partner).wait_recv()

    def sent(buf, ss, rs):
        rc(buf, buf, ss, rs, partner).wait_send()

    def f_copy(i):
        s = pl.ds(i * 512, 512)
        return pltpu.make_async_copy(facts_ref.at[s, :], fbuf.at[s, :], f_sem.at[i])

    for i in range(8):
        f_copy(i).start()

    ids = ids_ref[...]
    owner_hot = (lax.broadcasted_iota(jnp.int32, (16, ROWS), 0) == (ids >> 8)).astype(F32).astype(BF16)
    off_hot = (lax.broadcasted_iota(jnp.int32, (256, ROWS), 0) == (ids & 255)).astype(F32).astype(BF16)
    cnt[0] = lax.dot_general(owner_hot, off_hot, (((1,), (1,)), ((), ())), preferred_element_type=F32)

    pl.semaphore_wait(barrier, len(peers))

    def c_send(k, dev):
        rc(cnt.at[k], cland.at[k], c_s.at[k], c_r.at[k], dev).start()

    def c_take(k):
        arrived(cland.at[k], c_s.at[k], c_r.at[k])
        cnt[k + 1] = cnt[k] + cland[k]

    c_send(0, partner)

    for i in range(8):
        f_copy(i).wait()

        def split(j, c, i=i):
            s = rows(i * 512 + j * 128, 128)
            v = fbuf[s, :]
            h = v.astype(BF16)
            hl[s, 0:256] = h
            hl[s, 256:512] = (v - h.astype(F32)).astype(BF16)
            return c

        lax.fori_loop(0, 4, split, 0)

    x_even, y_even = x % 2 == 0, y % 2 == 0

    def pick(even, a, b):
        return {n: jnp.where(even, a[n], b[n]) for n in a}

    def count_step(k):
        c_take(k - 1)
        dev = (
            pick(x_even, xp, xm), pick(x_even, xm, xp), pick(y_even, yp, ym), pick(y_even, ym, yp)
        )[k - 1]
        c_send(k, dev)

    def count_z():
        c_take(4)
        for k in range(1, 8):
            zh, zl = z_peer(k)
            rc(cnt.at[5], czland.at[k - 1], cz_s.at[k - 1], cz_r.at[k - 1], at(zl=zl, zh=zh)).start()

    flipped = jnp.bitwise_xor(ids, core * 256)

    def compute(t, p, q):
        rel = jnp.where(q == 0, 2, jnp.where(q == 1, 1, jnp.where(q == 2, 3, 0)))
        zl = (z_lo + p) % 2
        base = (zl * 4 + (y + rel) % 4) * 512
        hot = (lax.broadcasted_iota(jnp.int32, (512, ROWS), 0) == (flipped - base)).astype(F32).astype(BF16)
        acc = jnp.dot(hot, hl[...], preferred_element_type=F32)
        own[t, 0] = acc[0:256, 0:128] + acc[0:256, 256:384]
        own[t, 1] = acc[0:256, 128:256] + acc[0:256, 384:512]
        part[t, 0] = acc[256:512, 0:128] + acc[256:512, 256:384]
        part[t, 1] = acc[256:512, 128:256] + acc[256:512, 384:512]
        rc(part.at[t], land.at[t], d_s.at[t], d_r.at[t], partner).start()

    def ring_x_a(buf, la, s, r):
        far = ((x + 2) % 4) * 64
        rc(buf.at[rows(far, 32), :], la.at[0], s.at[0], r.at[0], xp).start()
        rc(buf.at[rows(far + 32, 32), :], la.at[1], s.at[1], r.at[1], xm).start()

    def ring_x_b(buf, la, lb, sa, ra, sb, rb):
        nxt, prv = ((x + 1) % 4) * 64, ((x + 3) % 4) * 64
        arrived(la.at[0], sa.at[0], ra.at[0])
        s = rows(nxt, 32)
        buf[s, :] = buf[s, :] + la[0]
        rc(buf.at[rows(nxt, 64), :], lb.at[0], sb.at[0], rb.at[0], xp).start()
        arrived(la.at[1], sa.at[1], ra.at[1])
        s = rows(prv + 32, 32)
        buf[s, :] = buf[s, :] + la[1]
        rc(buf.at[rows(prv, 64), :], lb.at[1], sb.at[1], rb.at[1], xm).start()

    def ring_x_c(buf, lb, sb, rb):
        arrived(lb.at[0], sb.at[0], rb.at[0])
        arrived(lb.at[1], sb.at[1], rb.at[1])
        return buf[rows(x * 64, 64), :] + lb[0] + lb[1]

    def ring_y(buf, half, q, la, lb, sa, ra, sb, rb, done):
        lo, hi = pl.ds(0, half), pl.ds(half, half)

        def far():
            rc(buf.at[lo, :], la.at[0], sa.at[0], ra.at[0], yp).start()
            rc(buf.at[hi, :], la.at[1], sa.at[1], ra.at[1], ym).start()

        def nxt():
            arrived(la.at[0], sa.at[0], ra.at[0])
            buf[lo, :] = buf[lo, :] + la[0]
            rc(buf, lb.at[0], sb.at[0], rb.at[0], yp).start()

        def prv():
            arrived(la.at[1], sa.at[1], ra.at[1])
            buf[hi, :] = buf[hi, :] + la[1]
            rc(buf, lb.at[1], sb.at[1], rb.at[1], ym).start()

        def home():
            arrived(lb.at[0], sb.at[0], rb.at[0])
            arrived(lb.at[1], sb.at[1], rb.at[1])
            done(buf[...] + lb[0] + lb[1])

        for k, fn in enumerate((far, nxt, prv, home)):
            when(q == k, fn)

    def stage1(t, p, q):
        arrived(land.at[t], d_s.at[t], d_r.at[t])
        own[t, 0] = own[t, 0] + land[t, 0]
        ring_x_a(own.at[t, 0], xa.at[t], xa_s.at[t], xa_r.at[t])
        own[t, 1] = own[t, 1] + land[t, 1]

        def done(v):
            yr[p] = v
            ring_x_a(yr.at[p], yxa.at[p], yxa_s.at[p], yxa_r.at[p])

        ring_y(
            own.at[t, 1], 128, q, ya.at[p], yb.at[p], ya_s.at[p], ya_r.at[p], yb_s.at[p], yb_r.at[p], done
        )

    def stage2(t, p, q):
        ring_x_b(own.at[t, 0], xa.at[t], xb.at[t], xa_s.at[t], xa_r.at[t], xb_s.at[t], xb_r.at[t])

        def tail():
            ring_x_b(yr.at[p], yxa.at[p], yxb.at[p], yxa_s.at[p], yxa_r.at[p], yxb_s.at[p], yxb_r.at[p])

        when(q == 3, tail)

    my_z = z_hi * 2 + z_lo

    def stage3(t, p, q):
        xr[t] = ring_x_c(own.at[t, 0], xb.at[t], xb_s.at[t], xb_r.at[t])

        def done(v):
            fin[p, 0] = v
            fin[p, 1] = ring_x_c(yr.at[p], yxb.at[p], yxb_s.at[p], yxb_r.at[p])
            zl = (z_lo + p) % 2
            for k in range(4):
                zh = (z_hi + k) % 4

                def send(zh=zh, k=k):
                    rc(
                        fin.at[p, :, rows(zh * 16, 16), :], zl_buf.at[my_z], z_s.at[p * 4 + k],
                        z_r.at[my_z], at(zl=zl, zh=zh),
                    ).start()

                when((p == 1) if k == 0 else True, send)

        ring_y(
            xr.at[t], 32, q, xya.at[p], xyb.at[p], xya_s.at[p], xya_r.at[p], xyb_s.at[p], xyb_r.at[p], done
        )

    def step(t, c):
        for lag, stage in ((3, stage3), (2, stage2), (1, stage1)):

            def go(lag=lag, stage=stage):
                o = t - lag
                stage(o, o // 4, o % 4)

            when(t >= lag, go)
        for k in range(1, 5):
            when(t == k, functools.partial(count_step, k))
        when(t == 5, count_z)
        compute(t, t // 4, t % 4)
        return c

    lax.fori_loop(0, UNITS, step, 0)

    stage3(5, 1, 1)
    stage2(6, 1, 2)
    stage1(7, 1, 3)
    stage3(6, 1, 2)

    total = cnt[5]
    for k in range(7):
        arrived(czland.at[k], cz_s.at[k], cz_r.at[k])
        total = total + czland[k]
    row = jnp.sum(
        jnp.where(lax.broadcasted_iota(jnp.int32, (16, 256), 0) == dom, total, 0.0), axis=0, keepdims=True
    )
    mine = lax.broadcasted_iota(jnp.int32, (16, 256), 1) == (
        lax.broadcasted_iota(jnp.int32, (16, 256), 0) + rep * 16
    )
    column = jnp.sum(jnp.where(mine, row, 0.0), axis=1, keepdims=True)
    eye = lax.broadcasted_iota(jnp.int32, (16, 16), 0) == lax.broadcasted_iota(jnp.int32, (16, 16), 1)
    counts_ref[...] = jnp.sum(jnp.where(eye, column, 0.0), axis=0, keepdims=True)
    divisor = jnp.maximum(column, 1.0)

    stage2(7, 1, 3)
    stage3(7, 1, 3)

    mine_rows = rows(z_hi * 16, 16)
    left, right = fin[0, 0, mine_rows, :], fin[0, 1, mine_rows, :]
    for k in range(1, 8):
        zh, zl = z_peer(k)
        z = zh * 2 + zl
        arrived(zl_buf.at[z], z_s.at[0], z_r.at[z])
        left = left + zl_buf[z, 0]
        right = right + zl_buf[z, 1]
    means_ref[:, 0:128] = left / divisor
    means_ref[:, 128:256] = right / divisor

    def drain(t, c):
        sent(part.at[t], d_s.at[t], d_r.at[t])
        for k in range(2):
            sent(xa.at[t, k], xa_s.at[t, k], xa_r.at[t, k])
            sent(xb.at[t, k], xb_s.at[t, k], xb_r.at[t, k])
        return c

    lax.fori_loop(0, UNITS, drain, 0)
    for p in range(2):
        for k in range(2):
            for buf, s, r in (
                (ya, ya_s, ya_r), (yb, yb_s, yb_r), (yxa, yxa_s, yxa_r), (yxb, yxb_s, yxb_r),
                (xya, xya_s, xya_r), (xyb, xyb_s, xyb_r),
            ):
                sent(buf.at[p, k], s.at[p, k], r.at[p, k])
    for k in range(1, 8):
        sent(zl_buf.at[0], z_s.at[k], z_r.at[0])
    for k in range(5):
        sent(cland.at[k], c_s.at[k], c_r.at[k])
    for k in range(7):
        sent(czland.at[k], cz_s.at[k], cz_r.at[k])


def per_device(facts, row_owner, key_offset):
    ids = (row_owner[:, 0] * 256 + key_offset).reshape(1, ROWS)
    dma = pltpu.SemaphoreType.DMA
    vm = pltpu.VMEM
    means, counts = pl.pallas_call(
        kernel,
        out_shape=(jax.ShapeDtypeStruct((16, M), F32), jax.ShapeDtypeStruct((1, 16), F32)),
        in_specs=[pl.BlockSpec(memory_space=pltpu.VMEM), pl.BlockSpec(memory_space=pl.ANY)],
        out_specs=(pl.BlockSpec(memory_space=pltpu.VMEM), pl.BlockSpec(memory_space=pltpu.VMEM)),
        scratch_shapes=[
            vm((ROWS, M), F32), vm((ROWS, 2 * M), BF16),
            vm((8, 2, 256, 128), F32), vm((8, 2, 256, 128), F32), vm((8, 2, 256, 128), F32),
            vm((8, 2, 32, 128), F32), vm((8, 2, 64, 128), F32),
            vm((2, 2, 128, 128), F32), vm((2, 2, 256, 128), F32), vm((2, 256, 128), F32),
            vm((2, 2, 32, 128), F32), vm((2, 2, 64, 128), F32), vm((8, 64, 128), F32),
            vm((2, 2, 32, 128), F32), vm((2, 2, 64, 128), F32), vm((2, 2, 64, 128), F32),
            vm((8, 2, 16, 128), F32),
            vm((6, 16, 256), F32), vm((5, 16, 256), F32), vm((7, 16, 256), F32),
            dma((8,)), dma((8,)), dma((8,)),
            dma((8, 2)), dma((8, 2)), dma((8, 2)), dma((8, 2)),
            dma((2, 2)), dma((2, 2)), dma((2, 2)), dma((2, 2)),
            dma((2, 2)), dma((2, 2)), dma((2, 2)), dma((2, 2)),
            dma((2, 2)), dma((2, 2)), dma((2, 2)), dma((2, 2)),
            dma((8,)), dma((8,)), dma((5,)), dma((5,)), dma((7,)), dma((7,)),
        ],
        compiler_params=pltpu.CompilerParams(
            collective_id=0, has_side_effects=True, vmem_limit_bytes=56 * 1024 * 1024
        ),
    )(ids, facts)
    return means, counts.reshape(16)


def solution(mesh):
    placed = (P(("dom", "rep"), None), P(("dom", "rep"), None), P(("dom", "rep")))
    return jax.shard_map(
        per_device,
        mesh=mesh,
        in_specs=placed,
        out_specs=(P(("dom", "rep"), None), P(("dom", "rep"))),
        check_vma=False,
    )
```

```python
import jax
import jax.numpy as jnp
from jax import lax
from jax.experimental import pallas as pl
from jax.experimental.pallas import tpu as pltpu
from jax.sharding import PartitionSpec as P

MESH = pl.DeviceIdType.MESH
ROWS = 4096
KEYS = 4096
M = 256
UNITS = 8
F32 = jnp.float32
BF16 = jnp.bfloat16


def when(cond, fn):
    if isinstance(cond, (bool, int)):
        if cond:
            fn()
    else:
        pl.when(cond)(fn)


def rows(start, size):
    return pl.ds(pl.multiple_of(start, size), size)


def kernel(
    owner_ref, offset_ref, facts_ref, out_ref,
    ownbuf, offbuf, fbuf, hl, own, part, land, xa, xb, ya, yb, yr, yxa, yxb, xr, xya, xyb, fin, zl_buf,
    cnt, cnt_x, cnt_y, cx, cy, cz,
    i_sem, f_sem, d_s, d_r, xa_s, xa_r, xb_s, xb_r, ya_s, ya_r, yb_s, yb_r,
    yxa_s, yxa_r, yxb_s, yxb_r, xya_s, xya_r, xyb_s, xyb_r, z_s, z_r, cx_s, cx_r, cy_s, cy_r, cz_s, cz_r,
):
    dom, rep = lax.axis_index("dom"), lax.axis_index("rep")
    z_lo, y, core = dom // 8, (dom // 2) % 4, dom % 2
    x, z_hi = rep // 4, rep % 4

    def at(zl=z_lo, yy=y, cc=core, xx=x, zh=z_hi):
        return {"dom": zl * 8 + yy * 2 + cc, "rep": xx * 4 + zh}

    partner = at(cc=1 - core)
    xp, xm = at(xx=(x + 1) % 4), at(xx=(x + 3) % 4)
    yp, ym = at(yy=(y + 1) % 4), at(yy=(y + 3) % 4)

    def z_peer(k):
        z = (z_hi * 2 + z_lo + k) % 8
        return z // 2, z % 2

    peers = [partner]
    for k in range(1, 4):
        peers += [at(xx=(x + k) % 4), at(cc=1 - core, xx=(x + k) % 4), at(yy=(y + k) % 4)]
    for k in range(1, 8):
        zh, zl = z_peer(k)
        peers.append(at(zl=zl, zh=zh))

    barrier = pltpu.get_barrier_semaphore()
    for p in peers:
        pl.semaphore_signal(barrier, inc=1, device_id=p, device_id_type=MESH)

    def rc(src, dst, ss, rs, dev):
        return pltpu.make_async_remote_copy(
            src_ref=src, dst_ref=dst, send_sem=ss, recv_sem=rs, device_id=dev, device_id_type=MESH
        )

    def arrived(buf, ss, rs):
        rc(buf, buf, ss, rs, partner).wait_recv()

    def sent(buf, ss):
        rc(buf, buf, ss, d_r.at[0], partner).wait_send()

    def f_copy(i):
        s = pl.ds(i * 512, 512)
        return pltpu.make_async_copy(facts_ref.at[s, :], fbuf.at[s, :], f_sem.at[i])

    i_copies = (
        pltpu.make_async_copy(owner_ref, ownbuf, i_sem.at[0]),
        pltpu.make_async_copy(offset_ref, offbuf, i_sem.at[1]),
    )
    for c in i_copies:
        c.start()
    for i in range(8):
        f_copy(i).start()
    for c in i_copies:
        c.wait()

    owner, offset = ownbuf[...], offbuf[...]
    owner_hot = (lax.broadcasted_iota(jnp.int32, (16, ROWS), 0) == (owner % 2) * 8 + owner // 2).astype(F32).astype(BF16)
    off_hot = (lax.broadcasted_iota(jnp.int32, (256, ROWS), 0) == offset).astype(F32).astype(BF16)
    counts = lax.dot_general(owner_hot, off_hot, (((1,), (1,)), ((), ())), preferred_element_type=F32)
    cnt[0], cnt[1] = counts[0:8], counts[8:16]

    def count_x():
        for k in range(1, 8):
            cc, xx = (core + k // 4) % 2, (x + k) % 4
            rc(cnt.at[cc], cx.at[k - 1], cx_s, cx_r.at[k - 1], at(cc=cc, xx=xx)).start()

    def count_y():
        total = cnt[core]
        for k in range(7):
            arrived(cx.at[k], cx_s, cx_r.at[k])
            total = total + cx[k]
        cnt_x[...] = total
        for k in range(1, 4):
            rc(cnt_x, cy.at[k - 1], cy_s, cy_r.at[k - 1], at(yy=(y + k) % 4)).start()

    def count_z():
        total = cnt_x[...]
        for k in range(3):
            arrived(cy.at[k], cy_s, cy_r.at[k])
            total = total + cy[k]
        cnt_y[...] = total
        for k in range(1, 8):
            zh, zl = z_peer(k)
            rc(cnt_y, cz.at[k - 1], cz_s, cz_r.at[k - 1], at(zl=zl, zh=zh)).start()

    for i in range(8):
        f_copy(i).wait()

        def split(j, c, i=i):
            s = rows(i * 512 + j * 128, 128)
            v = fbuf[s, :]
            h = v.astype(BF16)
            hl[s, 0:256] = h
            hl[s, 256:512] = (v - h.astype(F32)).astype(BF16)
            return c

        lax.fori_loop(0, 4, split, 0)

    flipped = jnp.bitwise_xor(owner, core) * 256 + offset

    def order(t):
        p = jnp.where((t == 1) | (t == 4) | (t == 5) | (t == 7), 1, 0)
        q = jnp.where(t < 2, 0, jnp.where((t == 2) | (t == 4), 1, jnp.where(t < 6, 2, 3)))
        return p, q

    def keys_of(p, q):
        rel = jnp.where(q == 0, 2, jnp.where(q == 1, 1, jnp.where(q == 2, 3, 0)))
        return (((z_lo + p) % 2) * 4 + (y + rel) % 4) * 512

    def table(p, q, half):
        first = keys_of(p, q)
        k0 = half * (ROWS // 2)

        def one(k, size, m0=0, m=512, n0=0, n=512):
            keys = lax.broadcasted_iota(jnp.int32, (m, size), 0) + m0
            hot = (keys == (flipped[:, k : k + size] - first)).astype(F32).astype(BF16)
            return jnp.dot(hot, hl[k : k + size, n0 : n0 + n], preferred_element_type=F32)

        a, b = one(k0, 2048, 0, 256), one(k0, 2048, 256, 256)
        return jnp.concatenate([a[:, 0:256] + a[:, 256:512], b[:, 0:256] + b[:, 256:512]], axis=0)

    def first_half(t, p, q):
        v = table(p, q, 0)
        own[t, 0], own[t, 1] = v[0:256, 0:128], v[0:256, 128:256]
        part[t, 0], part[t, 1] = v[256:512, 0:128], v[256:512, 128:256]

    def second_half(t, p, q):
        v = table(p, q, 1)
        own[t, 0] = own[t, 0] + v[0:256, 0:128]
        own[t, 1] = own[t, 1] + v[0:256, 128:256]
        part[t, 0] = part[t, 0] + v[256:512, 0:128]
        part[t, 1] = part[t, 1] + v[256:512, 128:256]

    def swap(t):
        rc(part.at[t], land.at[t], d_s, d_r.at[t], partner).start()

    def ring_x_a(buf, la, s, r):
        far = ((x + 2) % 4) * 64
        rc(buf.at[rows(far, 32), :], la.at[0], s, r.at[0], xp).start()
        rc(buf.at[rows(far + 32, 32), :], la.at[1], s, r.at[1], xm).start()

    def ring_x_b(buf, la, lb, sa, ra, sb, rb):
        nxt, prv = ((x + 1) % 4) * 64, ((x + 3) % 4) * 64
        arrived(la.at[0], sa, ra.at[0])
        s = rows(nxt, 32)
        buf[s, :] = buf[s, :] + la[0]
        rc(buf.at[rows(nxt, 64), :], lb.at[0], sb, rb.at[0], xp).start()
        arrived(la.at[1], sa, ra.at[1])
        s = rows(prv + 32, 32)
        buf[s, :] = buf[s, :] + la[1]
        rc(buf.at[rows(prv, 64), :], lb.at[1], sb, rb.at[1], xm).start()

    def ring_x_c(buf, lb, sb, rb):
        arrived(lb.at[0], sb, rb.at[0])
        arrived(lb.at[1], sb, rb.at[1])
        return buf[rows(x * 64, 64), :] + lb[0] + lb[1]

    def ring_y(buf, half, q, la, lb, sa, ra, sb, rb, done):
        lo, hi = pl.ds(0, half), pl.ds(half, half)

        def far():
            rc(buf.at[lo, :], la.at[0], sa, ra.at[0], yp).start()
            rc(buf.at[hi, :], la.at[1], sa, ra.at[1], ym).start()

        def nxt():
            arrived(la.at[0], sa, ra.at[0])
            buf[lo, :] = buf[lo, :] + la[0]
            rc(buf, lb.at[0], sb, rb.at[0], yp).start()

        def prv():
            arrived(la.at[1], sa, ra.at[1])
            buf[hi, :] = buf[hi, :] + la[1]
            rc(buf, lb.at[1], sb, rb.at[1], ym).start()

        def home():
            arrived(lb.at[0], sb, rb.at[0])
            arrived(lb.at[1], sb, rb.at[1])
            done(buf[...] + lb[0] + lb[1])

        for k, fn in enumerate((far, nxt, prv, home)):
            when(q == k, fn)

    def stage1(t, p, q):
        arrived(land.at[t], d_s, d_r.at[t])
        own[t, 0] = own[t, 0] + land[t, 0]
        ring_x_a(own.at[t, 0], xa.at[t], xa_s, xa_r.at[t])
        own[t, 1] = own[t, 1] + land[t, 1]

        def done(v):
            yr[p] = v
            ring_x_a(yr.at[p], yxa.at[p], yxa_s, yxa_r.at[p])

        ring_y(
            own.at[t, 1], 128, q, ya.at[p], yb.at[p], ya_s, ya_r.at[p], yb_s, yb_r.at[p], done
        )

    def stage2(t, p, q):
        ring_x_b(own.at[t, 0], xa.at[t], xb.at[t], xa_s, xa_r.at[t], xb_s, xb_r.at[t])

        def tail():
            ring_x_b(yr.at[p], yxa.at[p], yxb.at[p], yxa_s, yxa_r.at[p], yxb_s, yxb_r.at[p])

        when(q == 3, tail)

    my_z = z_hi * 2 + z_lo

    def stage3(t, p, q):
        xr[t] = ring_x_c(own.at[t, 0], xb.at[t], xb_s, xb_r.at[t])

        def done(v):
            fin[p, 0] = v
            fin[p, 1] = ring_x_c(yr.at[p], yxb.at[p], yxb_s, yxb_r.at[p])
            zl = (z_lo + p) % 2
            for k in range(4):
                zh = (z_hi + k) % 4

                def send(zh=zh, k=k):
                    rc(
                        fin.at[p, :, rows(zh * 16, 16), :], zl_buf.at[my_z], z_s,
                        z_r.at[my_z], at(zl=zl, zh=zh),
                    ).start()

                when((p == 1) if k == 0 else True, send)

        ring_y(
            xr.at[t], 32, q, xya.at[p], xyb.at[p], xya_s, xya_r.at[p], xyb_s, xyb_r.at[p], done
        )

    first_half(0, 0, 0)
    second_half(0, 0, 0)
    pl.semaphore_wait(barrier, len(peers))
    swap(0)
    count_x()

    def late(stage, t):
        def go():
            stage(t, *order(t))

        when(t >= 0, go)

    def step(t, c):
        late(stage2, t - 3)
        when(t == 3, count_y)
        when(t == 5, count_z)
        first_half(t, *order(t))
        late(stage3, t - 4)
        late(stage1, t - 1)
        second_half(t, *order(t))
        swap(t)
        return c

    lax.fori_loop(1, UNITS, step, 0)

    stage2(5, 1, 2)
    stage3(4, 1, 1)
    stage1(7, 1, 3)
    stage2(6, 0, 3)
    stage3(5, 1, 2)

    total = cnt_y[...]
    for k in range(7):
        arrived(cz.at[k], cz_s, cz_r.at[k])
        total = total + cz[k]
    row = jnp.sum(
        jnp.where(lax.broadcasted_iota(jnp.int32, (8, 256), 0) == dom // 2, total, 0.0), axis=0, keepdims=True
    )
    mine = lax.broadcasted_iota(jnp.int32, (16, 256), 1) == (
        lax.broadcasted_iota(jnp.int32, (16, 256), 0) + rep * 16
    )
    column = jnp.sum(jnp.where(mine, row, 0.0), axis=1, keepdims=True)
    out_ref[:, 256:384] = jnp.broadcast_to(column, (16, 128))

    stage2(7, 1, 3)
    stage3(6, 0, 3)
    stage3(7, 1, 3)

    mine_rows = rows(z_hi * 16, 16)
    left, right = fin[0, 0, mine_rows, :], fin[0, 1, mine_rows, :]
    for k in range(1, 8):
        zh, zl = z_peer(k)
        z = zh * 2 + zl
        arrived(zl_buf.at[z], z_s, z_r.at[z])
        left = left + zl_buf[z, 0]
        right = right + zl_buf[z, 1]
    out_ref[:, 0:128] = left
    out_ref[:, 128:256] = right

    for buf, sem in (
        (part, d_s), (xa, xa_s), (xb, xb_s), (ya, ya_s), (yb, yb_s), (yxa, yxa_s), (yxb, yxb_s),
        (xya, xya_s), (xyb, xyb_s), (zl_buf.at[pl.ds(0, 7)], z_s), (cx, cx_s), (cy, cy_s), (cz, cz_s),
    ):
        sent(buf, sem)


def per_device(facts, row_owner, key_offset):
    dma = pltpu.SemaphoreType.DMA
    vm = pltpu.VMEM
    out = pl.pallas_call(
        kernel,
        out_shape=pltpu.VMEM((16, M + 128), F32),
        in_specs=[pl.BlockSpec(memory_space=pl.ANY)] * 3,
        out_specs=pl.BlockSpec(memory_space=vm),
        scratch_shapes=[
            vm((1, ROWS), jnp.int32), vm((1, ROWS), jnp.int32), vm((ROWS, M), F32), vm((ROWS, 2 * M), BF16),
            vm((8, 2, 256, 128), F32), vm((8, 2, 256, 128), F32), vm((8, 2, 256, 128), F32),
            vm((8, 2, 32, 128), F32), vm((8, 2, 64, 128), F32),
            vm((2, 2, 128, 128), F32), vm((2, 2, 256, 128), F32), vm((2, 256, 128), F32),
            vm((2, 2, 32, 128), F32), vm((2, 2, 64, 128), F32), vm((8, 64, 128), F32),
            vm((2, 2, 32, 128), F32), vm((2, 2, 64, 128), F32), vm((2, 2, 64, 128), F32),
            vm((8, 2, 16, 128), F32),
            vm((2, 8, 256), F32), vm((8, 256), F32), vm((8, 256), F32),
            vm((7, 8, 256), F32), vm((3, 8, 256), F32), vm((7, 8, 256), F32),
            dma((2,)), dma((8,)), dma, dma((8,)),
            dma, dma((8, 2)), dma, dma((8, 2)), dma, dma((2, 2)), dma, dma((2, 2)),
            dma, dma((2, 2)), dma, dma((2, 2)), dma, dma((2, 2)), dma, dma((2, 2)),
            dma, dma((8,)), dma, dma((7,)), dma, dma((3,)), dma, dma((7,)),
        ],
        compiler_params=pltpu.CompilerParams(
            collective_id=0, has_side_effects=True, vmem_limit_bytes=56 * 1024 * 1024
        ),
    )(row_owner.reshape(1, ROWS), key_offset.reshape(1, ROWS), facts)
    counts = out[:, M]
    return out[:, :M] / jnp.maximum(counts, 1.0)[:, None], counts


def solution(mesh):
    placed = (P(("dom", "rep"), None), P(("dom", "rep"), None), P(("dom", "rep")))
    return jax.shard_map(
        per_device,
        mesh=mesh,
        in_specs=placed,
        out_specs=(P(("dom", "rep"), None), P(("dom", "rep"))),
        check_vma=False,
    )
```

```python
import jax
import jax.numpy as jnp
from jax import lax
from jax.experimental import pallas as pl
from jax.experimental.pallas import tpu as pltpu
from jax.sharding import PartitionSpec as P

MESH = pl.DeviceIdType.MESH
ROWS = 4096
KEYS = 4096
M = 256
UNITS = 8
GROUPS = (
    ((2, 2), (1, 2), (2, 1), (3, 2)),
    ((2, 3), (0, 2), (2, 0), (1, 1)),
    ((1, 3), (3, 1), (3, 3), (0, 3)),
    ((0, 0), (0, 1), (1, 0), (3, 0)),
)
PLACE = {c: (g, i) for g, group in enumerate(GROUPS) for i, c in enumerate(group)}
F32 = jnp.float32
BF16 = jnp.bfloat16


def rows(start, size):
    return pl.ds(pl.multiple_of(start, size), size)


def kernel(
    owner_ref, offset_ref, facts_ref, means_ref, counts_ref,
    ownbuf, offbuf, fbuf, hl, own, part, land, fa, fb, res, sa, sb, fin, zl_buf,
    cnt, cnt_x, cnt_y, cx, cy, cz,
    i_sem, f_sem, d_s, d_r, fa_s, fa_r, fb_s, fb_r, sa_s, sa_r, sb_s, sb_r,
    z_s, z_r, cx_s, cx_r, cy_s, cy_r, cz_s, cz_r,
):
    dom, rep = lax.axis_index("dom"), lax.axis_index("rep")
    z_lo, y, core = dom // 8, (dom // 2) % 4, dom % 2
    x, z_hi = rep // 4, rep % 4

    def at(zl=z_lo, yy=y, cc=core, xx=x, zh=z_hi):
        return {"dom": zl * 8 + yy * 2 + cc, "rep": xx * 4 + zh}

    partner = at(cc=1 - core)
    xp, xm = at(xx=(x + 1) % 4), at(xx=(x + 3) % 4)
    yp, ym = at(yy=(y + 1) % 4), at(yy=(y + 3) % 4)

    def z_peer(k):
        z = (z_hi * 2 + z_lo + k) % 8
        return z // 2, z % 2

    peers = [partner]
    for k in range(1, 4):
        peers += [at(xx=(x + k) % 4), at(cc=1 - core, xx=(x + k) % 4), at(yy=(y + k) % 4)]
    for k in range(1, 8):
        zh, zl = z_peer(k)
        peers.append(at(zl=zl, zh=zh))

    def rc(src, dst, ss, rs, dev):
        return pltpu.make_async_remote_copy(
            src_ref=src, dst_ref=dst, send_sem=ss, recv_sem=rs, device_id=dev, device_id_type=MESH
        )

    def arrived(buf, ss, rs):
        rc(buf, buf, ss, rs, partner).wait_recv()

    def sent(buf, ss):
        rc(buf, buf, ss, d_r.at[0], partner).wait_send()

    def f_copy(i):
        s = pl.ds(i * 512, 512)
        return pltpu.make_async_copy(facts_ref.at[s, :], fbuf.at[s, :], f_sem.at[i])

    i_copies = (
        pltpu.make_async_copy(owner_ref, ownbuf, i_sem.at[0]),
        pltpu.make_async_copy(offset_ref, offbuf, i_sem.at[1]),
    )
    for c in i_copies:
        c.start()
    barrier = pltpu.get_barrier_semaphore()
    for p in peers:
        pl.semaphore_signal(barrier, inc=1, device_id=p, device_id_type=MESH)

    for i in range(8):
        f_copy(i).start()
    for c in i_copies:
        c.wait()

    owner, offset = ownbuf[...], offbuf[...]
    high = (owner % 2) * 16 + (owner // 2) * 2 + offset // 128
    high_hot = (lax.broadcasted_iota(jnp.int32, (32, ROWS), 0) == high).astype(F32).astype(BF16)
    low_hot = (lax.broadcasted_iota(jnp.int32, (128, ROWS), 0) == offset % 128).astype(F32).astype(BF16)
    counts = lax.dot_general(high_hot, low_hot, (((1,), (1,)), ((), ())), preferred_element_type=F32)
    cnt[0], cnt[1] = counts[0:16], counts[16:32]

    def count_x():
        for k in range(1, 8):
            cc, xx = (core + k // 4) % 2, (x + k) % 4
            rc(cnt.at[cc], cx.at[k - 1], cx_s, cx_r.at[k - 1], at(cc=cc, xx=xx)).start()

    def count_y():
        total = cnt[core]
        for k in range(7):
            arrived(cx.at[k], cx_s, cx_r.at[k])
            total = total + cx[k]
        cnt_x[...] = total
        for k in range(1, 4):
            rc(cnt_x, cy.at[k - 1], cy_s, cy_r.at[k - 1], at(yy=(y + k) % 4)).start()

    def count_z():
        total = cnt_x[...]
        for k in range(3):
            arrived(cy.at[k], cy_s, cy_r.at[k])
            total = total + cy[k]
        cnt_y[...] = total
        for k in range(1, 8):
            zh, zl = z_peer(k)
            rc(cnt_y, cz.at[k - 1], cz_s, cz_r.at[k - 1], at(zl=zl, zh=zh)).start()

    for i in range(8):
        f_copy(i).wait()

        def split(j, c, i=i):
            s = rows(i * 512 + j * 128, 128)
            v = fbuf[s, :]
            h = v.astype(BF16)
            hl[s, 0:256] = h
            hl[s, 256:512] = (v - h.astype(F32)).astype(BF16)
            return c

        lax.fori_loop(0, 4, split, 0)

    ids = owner * 256 + offset

    def table(t, half, of):
        g, p = t // 2, t % 2
        k = half * (ROWS // 2)
        part_ids = ids[:, k : k + ROWS // 2]
        keys = lax.broadcasted_iota(jnp.int32, (64, ROWS // 2), 0)
        hot = []
        for dx, dy in GROUPS[g]:
            dest = at(zl=(z_lo + p) % 2, yy=(y + dy) % 4, cc=of, xx=(x + dx) % 4, zh=0)
            hot.append((keys == part_ids - (dest["dom"] * 256 + dest["rep"] * 16)).astype(F32).astype(BF16))
        acc = jnp.dot(jnp.concatenate(hot, axis=0), hl[k : k + ROWS // 2, :], preferred_element_type=F32)
        return acc[:, 0:256] + acc[:, 256:512]

    def first_half(t):
        v, w = table(t, 0, core), table(t, 0, 1 - core)
        own[t, 0], own[t, 1] = v[:, 0:128], v[:, 128:256]
        part[t, 0], part[t, 1] = w[:, 0:128], w[:, 128:256]

    def second_half(t):
        v, w = table(t, 1, core), table(t, 1, 1 - core)
        own[t, 0] = own[t, 0] + v[:, 0:128]
        own[t, 1] = own[t, 1] + v[:, 128:256]
        part[t, 0] = part[t, 0] + w[:, 0:128]
        part[t, 1] = part[t, 1] + w[:, 128:256]

    def swap(t):
        rc(part.at[t], land.at[t], d_s, d_r.at[t], partner).start()

    along = ((xp, xm), (yp, ym))

    def block(k, p, d, e, start=0, size=64):
        g, i = PLACE[(d, e) if k == 0 else (e, d)]
        return own.at[2 * g + p, k, pl.ds(i * 64 + start, size), :]

    def add_in(buf, start, landed, ss, rs):
        arrived(landed, ss, rs)
        r = pl.ds(start, 32)
        buf[r, :] = buf[r, :] + landed[...]

    def far(k, p, e):
        for w in range(2):
            rc(block(k, p, 2, e, 32 * w, 32), fa.at[p, k, e, w], fa_s, fa_r.at[p, k, e, w], along[k][w]).start()

    def near(k, p, e, w):
        buf = block(k, p, 1 + 2 * w, e)
        add_in(buf, 32 * w, fa.at[p, k, e, w], fa_s, fa_r.at[p, k, e, w])
        rc(buf, fb.at[p, k, e, w], fb_s, fb_r.at[p, k, e, w], along[k][w]).start()

    def home(k, p, e):
        for w in range(2):
            arrived(fb.at[p, k, e, w], fb_s, fb_r.at[p, k, e, w])
        res[p, k, e] = block(k, p, 0, e)[...] + fb[p, k, e, 0] + fb[p, k, e, 1]

    def far2(k, p):
        for w in range(2):
            rc(res.at[p, k, 2, pl.ds(32 * w, 32), :], sa.at[p, k, w], sa_s, sa_r.at[p, k, w], along[1 - k][w]).start()

    def near2(k, p, w):
        buf = res.at[p, k, 1 + 2 * w]
        add_in(buf, 32 * w, sa.at[p, k, w], sa_s, sa_r.at[p, k, w])
        rc(buf, sb.at[p, k, w], sb_s, sb_r.at[p, k, w], along[1 - k][w]).start()

    def home2(k, p):
        for w in range(2):
            arrived(sb.at[p, k, w], sb_s, sb_r.at[p, k, w])
        fin[p, k] = res[p, k, 0] + sb[p, k, 0] + sb[p, k, 1]

    def join(t):
        arrived(land.at[t], d_s, d_r.at[t])
        own[t, 0] = own[t, 0] + land[t, 0]
        own[t, 1] = own[t, 1] + land[t, 1]

    def stage0(p):
        join(p)
        far(0, p, 2)
        far(1, p, 2)
        far(0, p, 1)
        far(1, p, 1)
        far(1, p, 3)

    def stage0b(p):
        near(0, p, 2, 0)
        near(0, p, 2, 1)
        near(1, p, 2, 0)

    def stage1(p):
        join(2 + p)
        far(0, p, 3)
        far(0, p, 0)
        far(1, p, 0)
        near(1, p, 2, 1)
        near(0, p, 1, 0)
        near(1, p, 1, 0)

    def stage2(p):
        join(4 + p)
        home(0, p, 2)
        far2(0, p)
        home(1, p, 2)
        far2(1, p)
        near(0, p, 1, 1)
        near(1, p, 1, 1)
        near(0, p, 3, 0)
        near(1, p, 3, 0)
        near(0, p, 3, 1)
        near(1, p, 3, 1)
        near(1, p, 0, 1)

    def stage2b(p):
        home(0, p, 3)
        near2(0, p, 1)

    def stage3(p):
        join(6 + p)
        near(0, p, 0, 0)
        near(0, p, 0, 1)
        near(1, p, 0, 0)
        home(1, p, 1)
        near2(1, p, 0)
        home(1, p, 3)
        near2(1, p, 1)
        home(0, p, 1)
        near2(0, p, 0)

    my_z = z_hi * 2 + z_lo

    def last(p):
        for k in range(2):
            home(k, p, 0)
            home2(k, p)
        for k in range(1 - p, 4):
            zh = (z_hi + k) % 4
            rc(
                fin.at[p, :, rows(zh * 16, 16), :], zl_buf.at[my_z], z_s, z_r.at[my_z],
                at(zl=(z_lo + p) % 2, zh=zh),
            ).start()

    stages = (stage0, stage1, stage2, stage3)
    early = {3: (stage0b, 0), 4: (stage0b, 1), 7: (stage2b, 0)}
    for t in range(UNITS):
        if t in early:
            early[t][0](early[t][1])
        if t == 3:
            count_y()
        if t == 5:
            count_z()
        first_half(t)
        if t:
            stages[(t - 1) // 2]((t - 1) % 2)
        second_half(t)
        if t == 0:
            pl.semaphore_wait(barrier, len(peers))
        swap(t)
        if t == 0:
            count_x()

    stage2b(1)
    stage3(1)

    total = cnt_y[...]
    for k in range(7):
        arrived(cz.at[k], cz_s, cz_r.at[k])
        total = total + cz[k]
    row = jnp.sum(
        jnp.where(lax.broadcasted_iota(jnp.int32, (16, 128), 0) == (dom // 2) * 2 + x // 2, total, 0.0),
        axis=0, keepdims=True,
    )
    mine = lax.broadcasted_iota(jnp.int32, (16, 128), 1) == (
        lax.broadcasted_iota(jnp.int32, (16, 128), 0) + (x % 2) * 64 + z_hi * 16
    )
    column = jnp.sum(jnp.where(mine, row, 0.0), axis=1, keepdims=True)
    eye = lax.broadcasted_iota(jnp.int32, (16, 16), 0) == lax.broadcasted_iota(jnp.int32, (16, 16), 1)
    counts_ref[...] = jnp.sum(jnp.where(eye, column, 0.0), axis=0, keepdims=True)
    divisor = jnp.maximum(column, 1.0)

    last(0)
    last(1)

    mine_rows = rows(z_hi * 16, 16)
    left, right = fin[0, 0, mine_rows, :], fin[0, 1, mine_rows, :]
    for k in range(1, 8):
        zh, zl = z_peer(k)
        z = zh * 2 + zl
        arrived(zl_buf.at[z], z_s, z_r.at[z])
        left = left + zl_buf[z, 0]
        right = right + zl_buf[z, 1]
    means_ref[:, 0:128] = left / divisor
    means_ref[:, 128:256] = right / divisor

    for buf, sem in (
        (part, d_s), (fa, fa_s), (fb, fb_s), (sa, sa_s), (sb, sb_s),
        (zl_buf.at[pl.ds(0, 7)], z_s), (cx, cx_s), (cy, cy_s), (cz, cz_s),
    ):
        sent(buf, sem)


def per_device(facts, row_owner, key_offset):
    dma = pltpu.SemaphoreType.DMA
    vm = pltpu.VMEM
    means, counts = pl.pallas_call(
        kernel,
        out_shape=(pltpu.VMEM((16, M), F32), pltpu.VMEM((1, 16), F32)),
        in_specs=[pl.BlockSpec(memory_space=pl.ANY)] * 3,
        out_specs=(pl.BlockSpec(memory_space=vm), pl.BlockSpec(memory_space=vm)),
        scratch_shapes=[
            vm((1, ROWS), jnp.int32), vm((1, ROWS), jnp.int32), vm((ROWS, M), F32), vm((ROWS, 2 * M), BF16),
            vm((8, 2, 256, 128), F32), vm((8, 2, 256, 128), F32), vm((8, 2, 256, 128), F32),
            vm((2, 2, 4, 2, 32, 128), F32), vm((2, 2, 4, 2, 64, 128), F32), vm((2, 2, 4, 64, 128), F32),
            vm((2, 2, 2, 32, 128), F32), vm((2, 2, 2, 64, 128), F32), vm((2, 2, 64, 128), F32),
            vm((8, 2, 16, 128), F32),
            vm((2, 16, 128), F32), vm((16, 128), F32), vm((16, 128), F32),
            vm((7, 16, 128), F32), vm((3, 16, 128), F32), vm((7, 16, 128), F32),
            dma((2,)), dma((8,)), dma, dma((8,)),
            dma, dma((2, 2, 4, 2)), dma, dma((2, 2, 4, 2)), dma, dma((2, 2, 2)), dma, dma((2, 2, 2)),
            dma, dma((8,)), dma, dma((7,)), dma, dma((3,)), dma, dma((7,)),
        ],
        compiler_params=pltpu.CompilerParams(
            collective_id=0, has_side_effects=True, vmem_limit_bytes=56 * 1024 * 1024
        ),
    )(row_owner.reshape(1, ROWS), key_offset.reshape(1, ROWS), facts)
    return means, counts.reshape(16)


def solution(mesh):
    placed = (P(("dom", "rep"), None), P(("dom", "rep"), None), P(("dom", "rep")))
    return jax.shard_map(
        per_device,
        mesh=mesh,
        in_specs=placed,
        out_specs=(P(("dom", "rep"), None), P(("dom", "rep"))),
        check_vma=False,
    )
```

```python
import jax
import jax.numpy as jnp
from jax import lax
from jax.experimental import pallas as pl
from jax.experimental.pallas import tpu as pltpu
from jax.sharding import PartitionSpec as P

MESH = pl.DeviceIdType.MESH
ROWS = 4096
KEYS = 4096
M = 256
UNITS = 8
GROUPS = (
    ((2, 2), (1, 2), (2, 1), (3, 2)),
    ((2, 3), (0, 2), (2, 0), (1, 1)),
    ((1, 3), (3, 1), (3, 3), (0, 3)),
    ((0, 0), (0, 1), (1, 0), (3, 0)),
)
PLACE = {c: (g, i) for g, group in enumerate(GROUPS) for i, c in enumerate(group)}
F32 = jnp.float32
BF16 = jnp.bfloat16
F8 = jnp.float8_e4m3fn


def rows(start, size):
    return pl.ds(pl.multiple_of(start, size), size)


def kernel(
    owner_ref, offset_ref, facts_ref, means_ref, counts_ref,
    ownbuf, offbuf, fbuf, hl, own, part, land, fa, fb, res, sa, sb, fin, zl_buf,
    cnt, cnt_x, cnt_y, cx, cy, cz,
    i_sem, f_sem, d_s, d_r, fa_s, fa_r, fb_s, fb_r, sa_s, sa_r, sb_s, sb_r,
    z_s, z_r, cx_s, cx_r, cy_s, cy_r, cz_s, cz_r,
):
    dom, rep = lax.axis_index("dom"), lax.axis_index("rep")
    z_lo, y, core = dom // 8, (dom // 2) % 4, dom % 2
    x, z_hi = rep // 4, rep % 4

    def at(zl=z_lo, yy=y, cc=core, xx=x, zh=z_hi):
        return {"dom": zl * 8 + yy * 2 + cc, "rep": xx * 4 + zh}

    partner = at(cc=1 - core)
    xp, xm = at(xx=(x + 1) % 4), at(xx=(x + 3) % 4)
    yp, ym = at(yy=(y + 1) % 4), at(yy=(y + 3) % 4)

    def z_peer(k):
        z = (z_hi * 2 + z_lo + k) % 8
        return z // 2, z % 2

    peers = [partner]
    for k in range(1, 4):
        peers += [at(xx=(x + k) % 4), at(cc=1 - core, xx=(x + k) % 4), at(yy=(y + k) % 4)]
    for k in range(1, 8):
        zh, zl = z_peer(k)
        peers.append(at(zl=zl, zh=zh))

    def rc(src, dst, ss, rs, dev):
        return pltpu.make_async_remote_copy(
            src_ref=src, dst_ref=dst, send_sem=ss, recv_sem=rs, device_id=dev, device_id_type=MESH
        )

    def arrived(buf, ss, rs):
        rc(buf, buf, ss, rs, partner).wait_recv()

    def sent(buf, ss):
        rc(buf, buf, ss, d_r.at[0], partner).wait_send()

    def f_copy(i):
        s = pl.ds(i * 512, 512)
        return pltpu.make_async_copy(facts_ref.at[s, :], fbuf.at[s, :], f_sem.at[i])

    i_copies = (
        pltpu.make_async_copy(owner_ref, ownbuf, i_sem.at[0]),
        pltpu.make_async_copy(offset_ref, offbuf, i_sem.at[1]),
    )
    for c in i_copies:
        c.start()
    barrier = pltpu.get_barrier_semaphore()
    for p in peers:
        pl.semaphore_signal(barrier, inc=1, device_id=p, device_id_type=MESH)

    for i in range(8):
        f_copy(i).start()
    for c in i_copies:
        c.wait()

    owner, offset = ownbuf[...], offbuf[...]
    high = (owner % 2) * 16 + (owner // 2) * 2 + offset // 128
    high_hot = (lax.broadcasted_iota(jnp.int32, (32, ROWS), 0) == high).astype(F32).astype(BF16)
    low_hot = (lax.broadcasted_iota(jnp.int32, (128, ROWS), 0) == offset % 128).astype(F32).astype(BF16)
    counts = lax.dot_general(high_hot, low_hot, (((1,), (1,)), ((), ())), preferred_element_type=F32)
    cnt[0], cnt[1] = counts[0:16], counts[16:32]

    def count_x():
        for k in range(1, 8):
            cc, xx = (core + k // 4) % 2, (x + k) % 4
            rc(cnt.at[cc], cx.at[k - 1], cx_s, cx_r.at[k - 1], at(cc=cc, xx=xx)).start()

    def count_y():
        total = cnt[core]
        for k in range(7):
            arrived(cx.at[k], cx_s, cx_r.at[k])
            total = total + cx[k]
        cnt_x[...] = total
        for k in range(1, 4):
            rc(cnt_x, cy.at[k - 1], cy_s, cy_r.at[k - 1], at(yy=(y + k) % 4)).start()

    def count_z():
        total = cnt_x[...]
        for k in range(3):
            arrived(cy.at[k], cy_s, cy_r.at[k])
            total = total + cy[k]
        cnt_y[...] = total
        for k in range(1, 8):
            zh, zl = z_peer(k)
            rc(cnt_y, cz.at[k - 1], cz_s, cz_r.at[k - 1], at(zl=zl, zh=zh)).start()

    top = jnp.zeros((8, 256), F32)
    for i in range(8):
        f_copy(i).wait()

        def peak(j, c, i=i):
            v = jnp.abs(fbuf[rows(i * 512 + j * 256, 256), :])
            return jnp.maximum(c, jnp.max(v.reshape(32, 8, 256), axis=0))

        top = lax.fori_loop(0, 2, peak, top)
    top = jnp.max(jnp.max(top, axis=0, keepdims=True), axis=1, keepdims=True)
    scale = jnp.minimum(256.0 / top, 2.0**126)
    unscale = 1.0 / scale

    def split(j, c):
        s = rows(j * 128, 128)
        v = fbuf[s, :] * scale
        for k in range(3):
            h = v.astype(F8)
            hl[s, k * 256 : (k + 1) * 256] = h
            v = (v - h.astype(F32)) * 16.0
        return c

    lax.fori_loop(0, ROWS // 128, split, 0)

    ids = owner * 256 + offset

    def table(t, half, of):
        g, p = t // 2, t % 2
        k = half * (ROWS // 2)
        part_ids = ids[:, k : k + ROWS // 2]
        keys = lax.broadcasted_iota(jnp.int32, (64, ROWS // 2), 0)
        hot = []
        for dx, dy in GROUPS[g]:
            dest = at(zl=(z_lo + p) % 2, yy=(y + dy) % 4, cc=of, xx=(x + dx) % 4, zh=0)
            hot.append((keys == part_ids - (dest["dom"] * 256 + dest["rep"] * 16)).astype(F32).astype(F8))
        acc = jnp.dot(jnp.concatenate(hot, axis=0), hl[k : k + ROWS // 2, :], preferred_element_type=F32)
        return (acc[:, 0:256] + acc[:, 256:512] * (1 / 16) + acc[:, 512:768] * (1 / 256)) * unscale

    def first_half(t):
        v, w = table(t, 0, core), table(t, 0, 1 - core)
        own[t, 0], own[t, 1] = v[:, 0:128], v[:, 128:256]
        part[t, 0], part[t, 1] = w[:, 0:128], w[:, 128:256]

    def second_half(t):
        v, w = table(t, 1, core), table(t, 1, 1 - core)
        own[t, 0] = own[t, 0] + v[:, 0:128]
        own[t, 1] = own[t, 1] + v[:, 128:256]
        part[t, 0] = part[t, 0] + w[:, 0:128]
        part[t, 1] = part[t, 1] + w[:, 128:256]

    def swap(t):
        rc(part.at[t], land.at[t], d_s, d_r.at[t], partner).start()

    along = ((xp, xm), (yp, ym))

    def block(k, p, d, e, start=0, size=64):
        g, i = PLACE[(d, e) if k == 0 else (e, d)]
        return own.at[2 * g + p, k, pl.ds(i * 64 + start, size), :]

    def add_in(buf, start, landed, ss, rs):
        arrived(landed, ss, rs)
        r = pl.ds(start, 32)
        buf[r, :] = buf[r, :] + landed[...]

    def far(k, p, e):
        for w in range(2):
            rc(block(k, p, 2, e, 32 * w, 32), fa.at[p, k, e, w], fa_s, fa_r.at[p, k, e, w], along[k][w]).start()

    def near(k, p, e, w):
        buf = block(k, p, 1 + 2 * w, e)
        add_in(buf, 32 * w, fa.at[p, k, e, w], fa_s, fa_r.at[p, k, e, w])
        rc(buf, fb.at[p, k, e, w], fb_s, fb_r.at[p, k, e, w], along[k][w]).start()

    def home(k, p, e):
        for w in range(2):
            arrived(fb.at[p, k, e, w], fb_s, fb_r.at[p, k, e, w])
        res[p, k, e] = block(k, p, 0, e)[...] + fb[p, k, e, 0] + fb[p, k, e, 1]

    def far2(k, p):
        for w in range(2):
            rc(res.at[p, k, 2, pl.ds(32 * w, 32), :], sa.at[p, k, w], sa_s, sa_r.at[p, k, w], along[1 - k][w]).start()

    def near2(k, p, w):
        buf = res.at[p, k, 1 + 2 * w]
        add_in(buf, 32 * w, sa.at[p, k, w], sa_s, sa_r.at[p, k, w])
        rc(buf, sb.at[p, k, w], sb_s, sb_r.at[p, k, w], along[1 - k][w]).start()

    def home2(k, p):
        for w in range(2):
            arrived(sb.at[p, k, w], sb_s, sb_r.at[p, k, w])
        fin[p, k] = res[p, k, 0] + sb[p, k, 0] + sb[p, k, 1]

    def join(t):
        arrived(land.at[t], d_s, d_r.at[t])
        own[t, 0] = own[t, 0] + land[t, 0]
        own[t, 1] = own[t, 1] + land[t, 1]

    def stage0(p):
        join(p)
        far(0, p, 2)
        far(1, p, 2)
        far(0, p, 1)
        far(1, p, 1)
        far(1, p, 3)

    def stage0b(p):
        near(0, p, 2, 0)
        near(0, p, 2, 1)
        near(1, p, 2, 0)

    def stage1(p):
        join(2 + p)
        far(0, p, 3)
        far(0, p, 0)
        far(1, p, 0)
        near(1, p, 2, 1)
        near(0, p, 1, 0)
        near(1, p, 1, 0)

    def stage2(p):
        join(4 + p)
        home(0, p, 2)
        far2(0, p)
        home(1, p, 2)
        far2(1, p)
        near(0, p, 1, 1)
        near(1, p, 1, 1)
        near(0, p, 3, 0)
        near(1, p, 3, 0)
        near(0, p, 3, 1)
        near(1, p, 3, 1)
        near(1, p, 0, 1)

    def stage2b(p):
        home(0, p, 3)
        near2(0, p, 1)

    def stage3(p):
        join(6 + p)
        near(0, p, 0, 0)
        near(0, p, 0, 1)
        near(1, p, 0, 0)
        home(1, p, 1)
        near2(1, p, 0)
        home(1, p, 3)
        near2(1, p, 1)
        home(0, p, 1)
        near2(0, p, 0)

    my_z = z_hi * 2 + z_lo

    def last(p):
        for k in range(2):
            home(k, p, 0)
            home2(k, p)
        for k in range(1 - p, 4):
            zh = (z_hi + k) % 4
            rc(
                fin.at[p, :, rows(zh * 16, 16), :], zl_buf.at[my_z], z_s, z_r.at[my_z],
                at(zl=(z_lo + p) % 2, zh=zh),
            ).start()

    stages = (stage0, stage1, stage2, stage3)
    def before(t):
        if t >= 2:
            if t in (4, 5):
                stage0b(t - 4)
            stages[(t - 2) // 2](t % 2)
        if t == 3:
            count_y()
        if t == 5:
            count_z()

    for t in range(UNITS - 1):
        before(t)
        first_half(t)
        second_half(t)
        if t == 0:
            pl.semaphore_wait(barrier, len(peers))
        swap(t)
        if t == 0:
            count_x()
    before(7)
    w0, w1 = table(7, 0, 1 - core), table(7, 1, 1 - core)
    part[7, 0], part[7, 1] = w0[:, 0:128] + w1[:, 0:128], w0[:, 128:256] + w1[:, 128:256]
    swap(7)
    stage2b(0)
    stage3(0)
    v0, v1 = table(7, 0, core), table(7, 1, core)
    own[7, 0], own[7, 1] = v0[:, 0:128] + v1[:, 0:128], v0[:, 128:256] + v1[:, 128:256]

    stage2b(1)
    stage3(1)

    total = cnt_y[...]
    for k in range(7):
        arrived(cz.at[k], cz_s, cz_r.at[k])
        total = total + cz[k]
    row = jnp.sum(
        jnp.where(lax.broadcasted_iota(jnp.int32, (16, 128), 0) == (dom // 2) * 2 + x // 2, total, 0.0),
        axis=0, keepdims=True,
    )
    mine = lax.broadcasted_iota(jnp.int32, (16, 128), 1) == (
        lax.broadcasted_iota(jnp.int32, (16, 128), 0) + (x % 2) * 64 + z_hi * 16
    )
    column = jnp.sum(jnp.where(mine, row, 0.0), axis=1, keepdims=True)
    eye = lax.broadcasted_iota(jnp.int32, (16, 16), 0) == lax.broadcasted_iota(jnp.int32, (16, 16), 1)
    counts_ref[...] = jnp.sum(jnp.where(eye, column, 0.0), axis=0, keepdims=True)
    divisor = jnp.maximum(column, 1.0)

    last(0)
    last(1)

    mine_rows = rows(z_hi * 16, 16)
    left, right = fin[0, 0, mine_rows, :], fin[0, 1, mine_rows, :]
    for k in range(1, 8):
        zh, zl = z_peer(k)
        z = zh * 2 + zl
        arrived(zl_buf.at[z], z_s, z_r.at[z])
        left = left + zl_buf[z, 0]
        right = right + zl_buf[z, 1]
    means_ref[:, 0:128] = left / divisor
    means_ref[:, 128:256] = right / divisor

    for buf, sem in (
        (part, d_s), (fa, fa_s), (fb, fb_s), (sa, sa_s), (sb, sb_s),
        (zl_buf.at[pl.ds(0, 7)], z_s), (cx, cx_s), (cy, cy_s), (cz, cz_s),
    ):
        sent(buf, sem)


def per_device(facts, row_owner, key_offset):
    dma = pltpu.SemaphoreType.DMA
    vm = pltpu.VMEM
    means, counts = pl.pallas_call(
        kernel,
        out_shape=(pltpu.VMEM((16, M), F32), pltpu.VMEM((1, 16), F32)),
        in_specs=[pl.BlockSpec(memory_space=pl.ANY)] * 3,
        out_specs=(pl.BlockSpec(memory_space=vm), pl.BlockSpec(memory_space=vm)),
        scratch_shapes=[
            vm((1, ROWS), jnp.int32), vm((1, ROWS), jnp.int32), vm((ROWS, M), F32), vm((ROWS, 3 * M), F8),
            vm((8, 2, 256, 128), F32), vm((8, 2, 256, 128), F32), vm((8, 2, 256, 128), F32),
            vm((2, 2, 4, 2, 32, 128), F32), vm((2, 2, 4, 2, 64, 128), F32), vm((2, 2, 4, 64, 128), F32),
            vm((2, 2, 2, 32, 128), F32), vm((2, 2, 2, 64, 128), F32), vm((2, 2, 64, 128), F32),
            vm((8, 2, 16, 128), F32),
            vm((2, 16, 128), F32), vm((16, 128), F32), vm((16, 128), F32),
            vm((7, 16, 128), F32), vm((3, 16, 128), F32), vm((7, 16, 128), F32),
            dma((2,)), dma((8,)), dma, dma((8,)),
            dma, dma((2, 2, 4, 2)), dma, dma((2, 2, 4, 2)), dma, dma((2, 2, 2)), dma, dma((2, 2, 2)),
            dma, dma((8,)), dma, dma((7,)), dma, dma((3,)), dma, dma((7,)),
        ],
        compiler_params=pltpu.CompilerParams(
            collective_id=0, has_side_effects=True, vmem_limit_bytes=56 * 1024 * 1024
        ),
    )(row_owner.reshape(1, ROWS), key_offset.reshape(1, ROWS), facts)
    return means, counts.reshape(16)


def solution(mesh):
    placed = (P(("dom", "rep"), None), P(("dom", "rep"), None), P(("dom", "rep")))
    return jax.shard_map(
        per_device,
        mesh=mesh,
        in_specs=placed,
        out_specs=(P(("dom", "rep"), None), P(("dom", "rep"))),
        check_vma=False,
    )
```

```python
import jax
import jax.numpy as jnp
from jax import lax
from jax.experimental import pallas as pl
from jax.experimental.pallas import tpu as pltpu
from jax.sharding import PartitionSpec as P

MESH = pl.DeviceIdType.MESH
ROWS = 4096
KEYS = 4096
M = 256
UNITS = 8
GROUPS = (
    ((2, 2), (1, 2), (2, 1), (3, 2)),
    ((2, 3), (0, 2), (2, 0), (1, 1)),
    ((1, 3), (3, 1), (3, 3), (0, 3)),
    ((0, 0), (0, 1), (1, 0), (3, 0)),
)
PLACE = {c: (g, i) for g, group in enumerate(GROUPS) for i, c in enumerate(group)}
F32 = jnp.float32
BF16 = jnp.bfloat16
F8 = jnp.float8_e4m3fn


def rows(start, size):
    return pl.ds(pl.multiple_of(start, size), size)


def kernel(
    owner_ref, offset_ref, facts_ref, means_ref, counts_ref,
    ownbuf, offbuf, fbuf, hl, own, part, land, fa, fb, res, sa, sb, fin, zl_buf,
    cnt, cnt_x, cnt_y, cx, cy, cz,
    i_sem, f_sem, d_s, d_r, fa_s, fa_r, fb_s, fb_r, sa_s, sa_r, sb_s, sb_r,
    z_s, z_r, cx_s, cx_r, cy_s, cy_r, cz_s, cz_r,
):
    dom, rep = lax.axis_index("dom"), lax.axis_index("rep")
    z_lo, y, core = dom // 8, (dom // 2) % 4, dom % 2
    x, z_hi = rep // 4, rep % 4

    def at(zl=z_lo, yy=y, cc=core, xx=x, zh=z_hi):
        return {"dom": zl * 8 + yy * 2 + cc, "rep": xx * 4 + zh}

    partner = at(cc=1 - core)
    xp, xm = at(xx=(x + 1) % 4), at(xx=(x + 3) % 4)
    yp, ym = at(yy=(y + 1) % 4), at(yy=(y + 3) % 4)

    def z_peer(k):
        z = (z_hi * 2 + z_lo + k) % 8
        return z // 2, z % 2

    peers = [partner]
    for k in range(1, 4):
        peers += [at(xx=(x + k) % 4), at(cc=1 - core, xx=(x + k) % 4), at(yy=(y + k) % 4)]
    for k in range(1, 8):
        zh, zl = z_peer(k)
        peers.append(at(zl=zl, zh=zh))

    def rc(src, dst, ss, rs, dev):
        return pltpu.make_async_remote_copy(
            src_ref=src, dst_ref=dst, send_sem=ss, recv_sem=rs, device_id=dev, device_id_type=MESH
        )

    def arrived(buf, ss, rs):
        rc(buf, buf, ss, rs, partner).wait_recv()

    def sent(buf, ss):
        rc(buf, buf, ss, d_r.at[0], partner).wait_send()

    def f_copy(i):
        s = pl.ds(i * 1024, 1024)
        return pltpu.make_async_copy(facts_ref.at[s, :], fbuf.at[s, :], f_sem.at[i])

    i_copies = (
        pltpu.make_async_copy(owner_ref, ownbuf, i_sem.at[0]),
        pltpu.make_async_copy(offset_ref, offbuf, i_sem.at[1]),
    )
    for c in i_copies:
        c.start()
    barrier = pltpu.get_barrier_semaphore()
    for p in peers:
        pl.semaphore_signal(barrier, inc=1, device_id=p, device_id_type=MESH)

    for i in range(4):
        f_copy(i).start()
    for c in i_copies:
        c.wait()

    owner, offset = ownbuf[...], offbuf[...]
    high = (owner % 2) * 16 + (owner // 2) * 2 + offset // 128
    high_hot = (lax.broadcasted_iota(jnp.int32, (32, ROWS), 0) == high).astype(F32).astype(BF16)
    low_hot = (lax.broadcasted_iota(jnp.int32, (128, ROWS), 0) == offset % 128).astype(F32).astype(BF16)
    counts = lax.dot_general(high_hot, low_hot, (((1,), (1,)), ((), ())), preferred_element_type=F32)
    cnt[0], cnt[1] = counts[0:16], counts[16:32]

    def count_x():
        for k in range(1, 8):
            cc, xx = (core + k // 4) % 2, (x + k) % 4
            rc(cnt.at[cc], cx.at[k - 1], cx_s, cx_r, at(cc=cc, xx=xx)).start()

    def count_y():
        total = cnt[core]
        arrived(cx, cx_s, cx_r)
        for k in range(7):
            total = total + cx[k]
        cnt_x[...] = total
        for k in range(1, 4):
            rc(cnt_x, cy.at[k - 1], cy_s, cy_r, at(yy=(y + k) % 4)).start()

    def count_z():
        total = cnt_x[...]
        arrived(cy, cy_s, cy_r)
        for k in range(3):
            total = total + cy[k]
        cnt_y[...] = total
        for k in range(1, 8):
            zh, zl = z_peer(k)
            rc(cnt_y, cz.at[k - 1], cz_s, cz_r, at(zl=zl, zh=zh)).start()

    top = jnp.zeros((8, 256), F32)
    for i in range(4):
        f_copy(i).wait()

        def peak(j, c, i=i):
            v = jnp.abs(fbuf[rows(i * 1024 + j * 256, 256), :])
            return jnp.maximum(c, jnp.max(v.reshape(32, 8, 256), axis=0))

        top = lax.fori_loop(0, 4, peak, top)
    top = jnp.max(jnp.max(top, axis=0, keepdims=True), axis=1, keepdims=True)
    scale = jnp.minimum(256.0 / top, 2.0**126)
    unscale = 1.0 / scale

    def split(j, c):
        s = rows(j * 128, 128)
        v = fbuf[s, :] * scale
        for k in range(3):
            h = v.astype(F8)
            hl[s, k * 256 : (k + 1) * 256] = h
            v = (v - h.astype(F32)) * 16.0
        return c

    lax.fori_loop(0, ROWS // 128, split, 0)

    ids = owner * 256 + offset

    def table(t, half, of):
        g, p = t // 2, t % 2
        k = half * (ROWS // 2)
        part_ids = ids[:, k : k + ROWS // 2]
        keys = lax.broadcasted_iota(jnp.int32, (64, ROWS // 2), 0)
        hot = []
        for dx, dy in GROUPS[g]:
            dest = at(zl=(z_lo + p) % 2, yy=(y + dy) % 4, cc=of, xx=(x + dx) % 4, zh=0)
            hot.append((keys == part_ids - (dest["dom"] * 256 + dest["rep"] * 16)).astype(F32).astype(F8))
        acc = jnp.dot(jnp.concatenate(hot, axis=0), hl[k : k + ROWS // 2, :], preferred_element_type=F32)
        return (acc[:, 0:256] + acc[:, 256:512] * (1 / 16) + acc[:, 512:768] * (1 / 256)) * unscale

    def first_half(t):
        v, w = table(t, 0, core), table(t, 0, 1 - core)
        own[t, 0], own[t, 1] = v[:, 0:128], v[:, 128:256]
        part[t, 0], part[t, 1] = w[:, 0:128], w[:, 128:256]

    def second_half(t):
        v, w = table(t, 1, core), table(t, 1, 1 - core)
        own[t, 0] = own[t, 0] + v[:, 0:128]
        own[t, 1] = own[t, 1] + v[:, 128:256]
        part[t, 0] = part[t, 0] + w[:, 0:128]
        part[t, 1] = part[t, 1] + w[:, 128:256]

    def swap(t):
        rc(part.at[t], land.at[t], d_s, d_r.at[t], partner).start()

    along = ((xp, xm), (yp, ym))

    def block(k, p, d, e, start=0, size=64):
        g, i = PLACE[(d, e) if k == 0 else (e, d)]
        return own.at[2 * g + p, k, pl.ds(i * 64 + start, size), :]

    waited = set()

    def both(name, buf, ss, rs):
        if name not in waited:
            waited.add(name)
            arrived(buf, ss, rs)

    def add_in(buf, start, landed):
        r = pl.ds(start, 32)
        buf[r, :] = buf[r, :] + landed[...]

    def far(k, p, e):
        for w in range(2):
            rc(block(k, p, 2, e, 32 * w, 32), fa.at[p, k, e, w], fa_s, fa_r.at[p, k, e], along[k][w]).start()

    def near(k, p, e, w):
        buf = block(k, p, 1 + 2 * w, e)
        both((0, p, k, e), fa.at[p, k, e], fa_s, fa_r.at[p, k, e])
        add_in(buf, 32 * w, fa.at[p, k, e, w])
        rc(buf, fb.at[p, k, e, w], fb_s, fb_r.at[p, k, e], along[k][w]).start()

    def home(k, p, e):
        arrived(fb.at[p, k, e], fb_s, fb_r.at[p, k, e])
        res[p, k, e] = block(k, p, 0, e)[...] + fb[p, k, e, 0] + fb[p, k, e, 1]

    def far2(k, p):
        for w in range(2):
            rc(res.at[p, k, 2, pl.ds(32 * w, 32), :], sa.at[p, k, w], sa_s, sa_r.at[p, k], along[1 - k][w]).start()

    def near2(k, p, w):
        buf = res.at[p, k, 1 + 2 * w]
        both((1, p, k), sa.at[p, k], sa_s, sa_r.at[p, k])
        add_in(buf, 32 * w, sa.at[p, k, w])
        rc(buf, sb.at[p, k, w], sb_s, sb_r.at[p, k], along[1 - k][w]).start()

    def home2(k, p):
        arrived(sb.at[p, k], sb_s, sb_r.at[p, k])
        fin[p, k] = res[p, k, 0] + sb[p, k, 0] + sb[p, k, 1]

    def join(t):
        arrived(land.at[t], d_s, d_r.at[t])
        own[t, 0] = own[t, 0] + land[t, 0]
        own[t, 1] = own[t, 1] + land[t, 1]

    def stage0(p):
        join(p)
        far(0, p, 2)
        far(1, p, 2)
        far(0, p, 1)
        far(1, p, 1)
        far(1, p, 3)

    def stage0b(p):
        near(0, p, 2, 0)
        near(0, p, 2, 1)
        near(1, p, 2, 0)

    def stage1(p):
        join(2 + p)
        far(0, p, 3)
        far(0, p, 0)
        far(1, p, 0)
        near(1, p, 2, 1)
        near(0, p, 1, 0)
        near(1, p, 1, 0)

    def stage2(p):
        join(4 + p)
        home(0, p, 2)
        far2(0, p)
        home(1, p, 2)
        far2(1, p)
        near(0, p, 1, 1)
        near(1, p, 1, 1)
        near(0, p, 3, 0)
        near(1, p, 3, 0)
        near(0, p, 3, 1)
        near(1, p, 3, 1)
        near(1, p, 0, 1)

    def stage2b(p):
        home(0, p, 3)
        near2(0, p, 1)

    def stage3(p):
        join(6 + p)
        near(0, p, 0, 0)
        near(0, p, 0, 1)
        near(1, p, 0, 0)
        home(1, p, 1)
        near2(1, p, 0)
        home(1, p, 3)
        near2(1, p, 1)
        home(0, p, 1)
        near2(0, p, 0)

    my_z = z_hi * 2 + z_lo

    def last(p):
        for k in range(2):
            home(k, p, 0)
            home2(k, p)
        for k in range(1 - p, 4):
            zh = (z_hi + k) % 4
            rc(
                fin.at[p, :, rows(zh * 16, 16), :], zl_buf.at[my_z], z_s, z_r,
                at(zl=(z_lo + p) % 2, zh=zh),
            ).start()

    stages = (stage0, stage1, stage2, stage3)
    def before(t):
        if t >= 2:
            if t in (4, 5):
                stage0b(t - 4)
            stages[(t - 2) // 2](t % 2)
        if t == 3:
            count_y()
        if t == 5:
            count_z()

    for t in range(UNITS - 1):
        before(t)
        first_half(t)
        second_half(t)
        if t == 0:
            pl.semaphore_wait(barrier, len(peers))
        swap(t)
        if t == 0:
            count_x()
    before(7)
    w0, w1 = table(7, 0, 1 - core), table(7, 1, 1 - core)
    part[7, 0], part[7, 1] = w0[:, 0:128] + w1[:, 0:128], w0[:, 128:256] + w1[:, 128:256]
    swap(7)
    stage2b(0)
    stage3(0)
    v0, v1 = table(7, 0, core), table(7, 1, core)
    own[7, 0], own[7, 1] = v0[:, 0:128] + v1[:, 0:128], v0[:, 128:256] + v1[:, 128:256]

    stage2b(1)
    stage3(1)

    total = cnt_y[...]
    arrived(cz, cz_s, cz_r)
    for k in range(7):
        total = total + cz[k]
    row = jnp.sum(
        jnp.where(lax.broadcasted_iota(jnp.int32, (16, 128), 0) == (dom // 2) * 2 + x // 2, total, 0.0),
        axis=0, keepdims=True,
    )
    mine = lax.broadcasted_iota(jnp.int32, (16, 128), 1) == (
        lax.broadcasted_iota(jnp.int32, (16, 128), 0) + (x % 2) * 64 + z_hi * 16
    )
    column = jnp.sum(jnp.where(mine, row, 0.0), axis=1, keepdims=True)
    eye = lax.broadcasted_iota(jnp.int32, (16, 16), 0) == lax.broadcasted_iota(jnp.int32, (16, 16), 1)
    counts_ref[...] = jnp.sum(jnp.where(eye, column, 0.0), axis=0, keepdims=True)
    divisor = jnp.maximum(column, 1.0)

    last(0)
    last(1)

    arrived(zl_buf.at[pl.ds(0, 7)], z_s, z_r)
    mine_rows = rows(z_hi * 16, 16)
    left, right = fin[0, 0, mine_rows, :], fin[0, 1, mine_rows, :]
    for k in range(1, 8):
        zh, zl = z_peer(k)
        z = zh * 2 + zl
        left = left + zl_buf[z, 0]
        right = right + zl_buf[z, 1]
    means_ref[:, 0:128] = left / divisor
    means_ref[:, 128:256] = right / divisor

    for buf, sem in (
        (part, d_s), (fa, fa_s), (fb, fb_s), (sa, sa_s), (sb, sb_s),
        (zl_buf.at[pl.ds(0, 7)], z_s), (cx, cx_s), (cy, cy_s), (cz, cz_s),
    ):
        sent(buf, sem)


def per_device(facts, row_owner, key_offset):
    dma = pltpu.SemaphoreType.DMA
    vm = pltpu.VMEM
    means, counts = pl.pallas_call(
        kernel,
        out_shape=(pltpu.VMEM((16, M), F32), pltpu.VMEM((1, 16), F32)),
        in_specs=[pl.BlockSpec(memory_space=pl.ANY)] * 3,
        out_specs=(pl.BlockSpec(memory_space=vm), pl.BlockSpec(memory_space=vm)),
        scratch_shapes=[
            vm((1, ROWS), jnp.int32), vm((1, ROWS), jnp.int32), vm((ROWS, M), F32), vm((ROWS, 3 * M), F8),
            vm((8, 2, 256, 128), F32), vm((8, 2, 256, 128), F32), vm((8, 2, 256, 128), F32),
            vm((2, 2, 4, 2, 32, 128), F32), vm((2, 2, 4, 2, 64, 128), F32), vm((2, 2, 4, 64, 128), F32),
            vm((2, 2, 2, 32, 128), F32), vm((2, 2, 2, 64, 128), F32), vm((2, 2, 64, 128), F32),
            vm((8, 2, 16, 128), F32),
            vm((2, 16, 128), F32), vm((16, 128), F32), vm((16, 128), F32),
            vm((7, 16, 128), F32), vm((3, 16, 128), F32), vm((7, 16, 128), F32),
            dma((2,)), dma((4,)), dma, dma((8,)),
            dma, dma((2, 2, 4)), dma, dma((2, 2, 4)), dma, dma((2, 2)), dma, dma((2, 2)),
            dma, dma, dma, dma, dma, dma, dma, dma,
        ],
        compiler_params=pltpu.CompilerParams(
            collective_id=0, has_side_effects=True, vmem_limit_bytes=56 * 1024 * 1024
        ),
    )(row_owner.reshape(1, ROWS), key_offset.reshape(1, ROWS), facts)
    return means, counts.reshape(16)


def solution(mesh):
    placed = (P(("dom", "rep"), None), P(("dom", "rep"), None), P(("dom", "rep")))
    return jax.shard_map(
        per_device,
        mesh=mesh,
        in_specs=placed,
        out_specs=(P(("dom", "rep"), None), P(("dom", "rep"))),
        check_vma=False,
    )
```

```python
import jax
import jax.numpy as jnp
from jax import lax
from jax.experimental import pallas as pl
from jax.experimental.pallas import tpu as pltpu
from jax.sharding import PartitionSpec as P

MESH = pl.DeviceIdType.MESH
ROWS = 4096
KEYS = 4096
M = 256
UNITS = 8
GROUPS = (
    ((2, 2), (1, 2), (2, 1), (3, 2)),
    ((2, 3), (0, 2), (2, 0), (1, 1)),
    ((1, 3), (3, 1), (3, 3), (0, 3)),
    ((0, 0), (0, 1), (1, 0), (3, 0)),
)
PLACE = {c: (g, i) for g, group in enumerate(GROUPS) for i, c in enumerate(group)}
FIRST = 1024
F32 = jnp.float32
BF16 = jnp.bfloat16
F8 = jnp.float8_e4m3fn


def rows(start, size):
    return pl.ds(pl.multiple_of(start, size), size)


def kernel(
    owner_ref, offset_ref, facts_ref, means_ref, counts_ref,
    ownbuf, offbuf, fbuf, hl, own, part, land, fa, fb, res, sa, sb, fin, zl_buf,
    cnt, cnt_x, cnt_y, cx, cy, cz,
    i_sem, f_sem, d_s, d_r, fa_s, fa_r, fb_s, fb_r, sa_s, sa_r, sb_s, sb_r,
    z_s, z_r, cx_s, cx_r, cy_s, cy_r, cz_s, cz_r,
):
    dom, rep = lax.axis_index("dom"), lax.axis_index("rep")
    z_lo, y, core = dom // 8, (dom // 2) % 4, dom % 2
    x, z_hi = rep // 4, rep % 4

    def at(zl=z_lo, yy=y, cc=core, xx=x, zh=z_hi):
        return {"dom": zl * 8 + yy * 2 + cc, "rep": xx * 4 + zh}

    partner = at(cc=1 - core)
    xp, xm = at(xx=(x + 1) % 4), at(xx=(x + 3) % 4)
    yp, ym = at(yy=(y + 1) % 4), at(yy=(y + 3) % 4)

    def z_peer(k):
        z = (z_hi * 2 + z_lo + k) % 8
        return z // 2, z % 2

    peers = [partner]
    for k in range(1, 4):
        peers += [at(xx=(x + k) % 4), at(cc=1 - core, xx=(x + k) % 4), at(yy=(y + k) % 4)]
    for k in range(1, 8):
        zh, zl = z_peer(k)
        peers.append(at(zl=zl, zh=zh))

    def rc(src, dst, ss, rs, dev):
        return pltpu.make_async_remote_copy(
            src_ref=src, dst_ref=dst, send_sem=ss, recv_sem=rs, device_id=dev, device_id_type=MESH
        )

    def arrived(buf, ss, rs):
        rc(buf, buf, ss, rs, partner).wait_recv()

    def sent(buf, ss):
        rc(buf, buf, ss, d_r.at[0], partner).wait_send()

    def f_copy(i):
        s = pl.ds(i * 1024, 1024)
        return pltpu.make_async_copy(facts_ref.at[s, :], fbuf.at[s, :], f_sem.at[i])

    i_copies = (
        pltpu.make_async_copy(owner_ref, ownbuf, i_sem.at[0]),
        pltpu.make_async_copy(offset_ref, offbuf, i_sem.at[1]),
    )
    for c in i_copies:
        c.start()
    barrier = pltpu.get_barrier_semaphore()
    for p in peers:
        pl.semaphore_signal(barrier, inc=1, device_id=p, device_id_type=MESH)

    for i in range(4):
        f_copy(i).start()
    for c in i_copies:
        c.wait()

    owner, offset = ownbuf[...], offbuf[...]
    high = (owner % 2) * 16 + (owner // 2) * 2 + offset // 128
    high_hot = (lax.broadcasted_iota(jnp.int32, (32, ROWS), 0) == high).astype(F32).astype(BF16)
    low_hot = (lax.broadcasted_iota(jnp.int32, (128, ROWS), 0) == offset % 128).astype(F32).astype(BF16)
    counts = lax.dot_general(high_hot, low_hot, (((1,), (1,)), ((), ())), preferred_element_type=F32)
    cnt[0], cnt[1] = counts[0:16], counts[16:32]

    def count_x():
        for k in range(1, 8):
            cc, xx = (core + k // 4) % 2, (x + k) % 4
            rc(cnt.at[cc], cx.at[k - 1], cx_s, cx_r, at(cc=cc, xx=xx)).start()

    def count_y():
        total = cnt[core]
        arrived(cx, cx_s, cx_r)
        for k in range(7):
            total = total + cx[k]
        cnt_x[...] = total
        for k in range(1, 4):
            rc(cnt_x, cy.at[k - 1], cy_s, cy_r, at(yy=(y + k) % 4)).start()

    def count_z():
        total = cnt_x[...]
        arrived(cy, cy_s, cy_r)
        for k in range(3):
            total = total + cy[k]
        cnt_y[...] = total
        for k in range(1, 8):
            zh, zl = z_peer(k)
            rc(cnt_y, cz.at[k - 1], cz_s, cz_r, at(zl=zl, zh=zh)).start()

    top = jnp.zeros((8, 256), F32)
    for i in range(4):
        f_copy(i).wait()

        def peak(j, c, i=i):
            v = jnp.abs(fbuf[rows(i * 1024 + j * 256, 256), :])
            return jnp.maximum(c, jnp.max(v.reshape(32, 8, 256), axis=0))

        top = lax.fori_loop(0, 4, peak, top)
    top = jnp.max(jnp.max(top, axis=0, keepdims=True), axis=1, keepdims=True)
    scale = jnp.minimum(256.0 / top, 2.0**126)
    unscale = 1.0 / scale

    def split(s):
        v = fbuf[s, :] * scale
        for k in range(3):
            h = v.astype(F8)
            hl[s, k * 256 : (k + 1) * 256] = h
            v = (v - h.astype(F32)) * 16.0

    def split_first(j, c):
        split(rows(j * 128, 128))
        return c

    lax.fori_loop(0, FIRST // 128, split_first, 0)

    ids = owner * 256 + offset

    def table(t, half, of, size=ROWS // 2):
        g, p = t // 2, t % 2
        k = half * size
        part_ids = ids[:, k : k + size]
        keys = lax.broadcasted_iota(jnp.int32, (64, size), 0)
        hot = []
        for dx, dy in GROUPS[g]:
            dest = at(zl=(z_lo + p) % 2, yy=(y + dy) % 4, cc=of, xx=(x + dx) % 4, zh=0)
            hot.append((keys == part_ids - (dest["dom"] * 256 + dest["rep"] * 16)).astype(F32).astype(F8))
        acc = jnp.dot(jnp.concatenate(hot, axis=0), hl[k : k + size, :], preferred_element_type=F32)
        return (acc[:, 0:256] + acc[:, 256:512] * (1 / 16) + acc[:, 512:768] * (1 / 256)) * unscale

    def first_half(t):
        v, w = table(t, 0, core), table(t, 0, 1 - core)
        own[t, 0], own[t, 1] = v[:, 0:128], v[:, 128:256]
        part[t, 0], part[t, 1] = w[:, 0:128], w[:, 128:256]

    def second_half(t):
        v, w = table(t, 1, core), table(t, 1, 1 - core)
        own[t, 0] = own[t, 0] + v[:, 0:128]
        own[t, 1] = own[t, 1] + v[:, 128:256]
        part[t, 0] = part[t, 0] + w[:, 0:128]
        part[t, 1] = part[t, 1] + w[:, 128:256]

    def swap(t):
        rc(part.at[t], land.at[t], d_s, d_r.at[t], partner).start()

    along = ((xp, xm), (yp, ym))

    def block(k, p, d, e, start=0, size=64):
        g, i = PLACE[(d, e) if k == 0 else (e, d)]
        return own.at[2 * g + p, k, pl.ds(i * 64 + start, size), :]

    waited = set()

    def both(name, buf, ss, rs):
        if name not in waited:
            waited.add(name)
            arrived(buf, ss, rs)

    def add_in(buf, start, landed):
        r = pl.ds(start, 32)
        buf[r, :] = buf[r, :] + landed[...]

    def far(k, p, e):
        for w in range(2):
            rc(block(k, p, 2, e, 32 * w, 32), fa.at[p, k, e, w], fa_s, fa_r.at[p, k, e], along[k][w]).start()

    def near(k, p, e, w):
        buf = block(k, p, 1 + 2 * w, e)
        both((0, p, k, e), fa.at[p, k, e], fa_s, fa_r.at[p, k, e])
        add_in(buf, 32 * w, fa.at[p, k, e, w])
        rc(buf, fb.at[p, k, e, w], fb_s, fb_r.at[p, k, e], along[k][w]).start()

    def home(k, p, e):
        arrived(fb.at[p, k, e], fb_s, fb_r.at[p, k, e])
        res[p, k, e] = block(k, p, 0, e)[...] + fb[p, k, e, 0] + fb[p, k, e, 1]

    def far2(k, p):
        for w in range(2):
            rc(res.at[p, k, 2, pl.ds(32 * w, 32), :], sa.at[p, k, w], sa_s, sa_r.at[p, k], along[1 - k][w]).start()

    def near2(k, p, w):
        buf = res.at[p, k, 1 + 2 * w]
        both((1, p, k), sa.at[p, k], sa_s, sa_r.at[p, k])
        add_in(buf, 32 * w, sa.at[p, k, w])
        rc(buf, sb.at[p, k, w], sb_s, sb_r.at[p, k], along[1 - k][w]).start()

    def home2(k, p):
        arrived(sb.at[p, k], sb_s, sb_r.at[p, k])
        fin[p, k] = res[p, k, 0] + sb[p, k, 0] + sb[p, k, 1]

    def join(t):
        arrived(land.at[t], d_s, d_r.at[t])
        own[t, 0] = own[t, 0] + land[t, 0]
        own[t, 1] = own[t, 1] + land[t, 1]

    def stage0(p):
        join(p)
        far(0, p, 2)
        far(1, p, 2)
        far(0, p, 1)
        far(1, p, 1)
        far(1, p, 3)

    def stage0b(p):
        near(0, p, 2, 0)
        near(0, p, 2, 1)
        near(1, p, 2, 0)

    def stage1(p):
        join(2 + p)
        far(0, p, 3)
        far(0, p, 0)
        far(1, p, 0)
        near(1, p, 2, 1)
        near(0, p, 1, 0)
        near(1, p, 1, 0)

    def stage2(p):
        join(4 + p)
        home(0, p, 2)
        far2(0, p)
        home(1, p, 2)
        far2(1, p)
        near(0, p, 1, 1)
        near(1, p, 1, 1)
        near(0, p, 3, 0)
        near(1, p, 3, 0)
        near(0, p, 3, 1)
        near(1, p, 3, 1)
        near(1, p, 0, 1)

    def stage2b(p):
        home(0, p, 3)
        near2(0, p, 1)

    def stage3(p):
        join(6 + p)
        near(0, p, 0, 0)
        near(0, p, 0, 1)
        near(1, p, 0, 0)
        stage2b(p)
        home(1, p, 1)
        near2(1, p, 0)
        home(1, p, 3)
        near2(1, p, 1)
        home(0, p, 1)
        near2(0, p, 0)

    my_z = z_hi * 2 + z_lo

    def last(p):
        for k in range(2):
            home(k, p, 0)
            home2(k, p)
        for k in range(1 - p, 4):
            zh = (z_hi + k) % 4
            rc(
                fin.at[p, :, rows(zh * 16, 16), :], zl_buf.at[my_z], z_s, z_r,
                at(zl=(z_lo + p) % 2, zh=zh),
            ).start()

    stages = (stage0, stage1, stage2, stage3)
    def before(t):
        if t >= 2:
            if t in (4, 5):
                stage0b(t - 4)
            stages[(t - 2) // 2](t % 2)
        if t == 3:
            count_y()
        if t == 5:
            count_z()

    for t in range(UNITS - 1):
        before(t)
        if t:
            first_half(t)
            second_half(t)
        else:
            for n in range(ROWS // FIRST):
                v, w = table(0, n, core, FIRST), table(0, n, 1 - core, FIRST)
                if n + 1 < ROWS // FIRST:
                    for m in range(0, FIRST, 128):
                        split(pl.ds((n + 1) * FIRST + m, 128))
                for c in range(2):
                    lanes = slice(128 * c, 128 * c + 128)
                    own[0, c] = v[:, lanes] if n == 0 else own[0, c] + v[:, lanes]
                    part[0, c] = w[:, lanes] if n == 0 else part[0, c] + w[:, lanes]
        if t == 0:
            pl.semaphore_wait(barrier, len(peers))
        swap(t)
        if t == 0:
            count_x()
    before(7)
    w0, w1 = table(7, 0, 1 - core), table(7, 1, 1 - core)
    part[7, 0], part[7, 1] = w0[:, 0:128] + w1[:, 0:128], w0[:, 128:256] + w1[:, 128:256]
    swap(7)
    stage3(0)
    v0, v1 = table(7, 0, core), table(7, 1, core)
    own[7, 0], own[7, 1] = v0[:, 0:128] + v1[:, 0:128], v0[:, 128:256] + v1[:, 128:256]

    stage3(1)

    total = cnt_y[...]
    arrived(cz, cz_s, cz_r)
    for k in range(7):
        total = total + cz[k]
    row = jnp.sum(
        jnp.where(lax.broadcasted_iota(jnp.int32, (16, 128), 0) == (dom // 2) * 2 + x // 2, total, 0.0),
        axis=0, keepdims=True,
    )
    mine = lax.broadcasted_iota(jnp.int32, (16, 128), 1) == (
        lax.broadcasted_iota(jnp.int32, (16, 128), 0) + (x % 2) * 64 + z_hi * 16
    )
    column = jnp.sum(jnp.where(mine, row, 0.0), axis=1, keepdims=True)
    eye = lax.broadcasted_iota(jnp.int32, (16, 16), 0) == lax.broadcasted_iota(jnp.int32, (16, 16), 1)
    counts_ref[...] = jnp.sum(jnp.where(eye, column, 0.0), axis=0, keepdims=True)
    divisor = jnp.maximum(column, 1.0)

    last(0)
    last(1)

    arrived(zl_buf.at[pl.ds(0, 7)], z_s, z_r)
    mine_rows = rows(z_hi * 16, 16)
    left, right = fin[0, 0, mine_rows, :], fin[0, 1, mine_rows, :]
    for k in range(1, 8):
        zh, zl = z_peer(k)
        z = zh * 2 + zl
        left = left + zl_buf[z, 0]
        right = right + zl_buf[z, 1]
    means_ref[:, 0:128] = left / divisor
    means_ref[:, 128:256] = right / divisor

    for buf, sem in (
        (part, d_s), (fa, fa_s), (fb, fb_s), (sa, sa_s), (sb, sb_s),
        (zl_buf.at[pl.ds(0, 7)], z_s), (cx, cx_s), (cy, cy_s), (cz, cz_s),
    ):
        sent(buf, sem)


def per_device(facts, row_owner, key_offset):
    dma = pltpu.SemaphoreType.DMA
    vm = pltpu.VMEM
    means, counts = pl.pallas_call(
        kernel,
        out_shape=(pltpu.VMEM((16, M), F32), pltpu.VMEM((1, 16), F32)),
        in_specs=[pl.BlockSpec(memory_space=pl.ANY)] * 3,
        out_specs=(pl.BlockSpec(memory_space=vm), pl.BlockSpec(memory_space=vm)),
        scratch_shapes=[
            vm((1, ROWS), jnp.int32), vm((1, ROWS), jnp.int32), vm((ROWS, M), F32), vm((ROWS, 3 * M), F8),
            vm((8, 2, 256, 128), F32), vm((8, 2, 256, 128), F32), vm((8, 2, 256, 128), F32),
            vm((2, 2, 4, 2, 32, 128), F32), vm((2, 2, 4, 2, 64, 128), F32), vm((2, 2, 4, 64, 128), F32),
            vm((2, 2, 2, 32, 128), F32), vm((2, 2, 2, 64, 128), F32), vm((2, 2, 64, 128), F32),
            vm((8, 2, 16, 128), F32),
            vm((2, 16, 128), F32), vm((16, 128), F32), vm((16, 128), F32),
            vm((7, 16, 128), F32), vm((3, 16, 128), F32), vm((7, 16, 128), F32),
            dma((2,)), dma((4,)), dma, dma((8,)),
            dma, dma((2, 2, 4)), dma, dma((2, 2, 4)), dma, dma((2, 2)), dma, dma((2, 2)),
            dma, dma, dma, dma, dma, dma, dma, dma,
        ],
        compiler_params=pltpu.CompilerParams(
            collective_id=0, has_side_effects=True, vmem_limit_bytes=56 * 1024 * 1024
        ),
    )(row_owner.reshape(1, ROWS), key_offset.reshape(1, ROWS), facts)
    return means, counts.reshape(16)


def solution(mesh):
    placed = (P(("dom", "rep"), None), P(("dom", "rep"), None), P(("dom", "rep")))
    return jax.shard_map(
        per_device,
        mesh=mesh,
        in_specs=placed,
        out_specs=(P(("dom", "rep"), None), P(("dom", "rep"))),
        check_vma=False,
    )
```
